256 devices in a mesh: seq: 64 (over z, y, core), head: 4 (over x).
Axes of the slice: x: 4, y: 4, z: 8, core: 2. Of those that a mesh axis runs over, the one named last changes fastest.
Arguments:
- queries: bfloat16 [16384, 4096], P('seq', 'head'), may hold values from -5 to 5
- keys: bfloat16 [16384, 4096], P('seq', 'head'), may hold values from -5 to 5
- values: bfloat16 [16384, 4096], P('seq', 'head'), may hold values from -6 to 6
- beta: float32 [32], P('head'), may hold values from -2 to 2
- w_out: bfloat16 [4096, 4096], P('head'), may hold values from -0.09375 to 0.09375
Outputs:
- mixed: bfloat16 [16384, 4096], P('seq', 'head')
The draws below stay inside these ranges and needn't reach their ends.
All inputs are finite; a program needn't handle non-finite values.
Results may differ from the reference program's by a relative error of at most 0.0069.
Values may be sent and summed in bfloat16 or wider, within the bound.
No kernel may reach another device: no remote copies, remote signals or barrier semaphores. Data moves between devices by JAX's collectives and lax.ppermute only.
A program may use at most 192 MiB of HBM per device.

```python
import jax
import jax.numpy as jnp
from jax import lax

D = 4096
HEADS = 32
HD = 128
SEG = 2048
TOKENS = 16384


def draw_queries(key, part):
    own_key = jax.random.fold_in(key, 11)
    extent = (TOKENS, HEADS * HD)
    base = jnp.clip(0.7 * jax.random.normal(own_key, extent, jnp.float32), -5.0, 5.0)
    return base.astype(jnp.bfloat16)


def draw_keys(key, part):
    own_key = jax.random.fold_in(key, 12)
    extent = (TOKENS, HEADS * HD)
    position = jnp.arange(TOKENS)
    rising = (3.0 * position.astype(jnp.float32) / TOKENS)[:, None]
    base = jnp.clip(jax.random.normal(own_key, extent, jnp.float32) + rising, -5.0, 5.0)
    return base.astype(jnp.bfloat16)


def draw_values(key, part):
    own_key = jax.random.fold_in(key, 13)
    extent = (TOKENS, HEADS * HD)
    segments = TOKENS // SEG
    offsets = jax.random.normal(jax.random.fold_in(key, 14), (segments, HEADS * HD), jnp.float32)
    noise = jax.random.normal(own_key, extent, jnp.float32)
    spread = jnp.repeat(offsets, SEG, axis=0)
    return jnp.clip(0.8 * noise + 0.8 * spread, -6.0, 6.0).astype(jnp.bfloat16)


def steps_of(key, shape, split, low, largest):
    loudness = 1.0
    for dim, shards_of in split:
        draws = jax.random.uniform(jax.random.fold_in(jax.random.fold_in(key, 6), dim), (shards_of,), jnp.float32, low / len(split), largest / len(split))
        loudness = loudness * jnp.repeat(jnp.exp(draws), shape[dim] // shards_of).reshape((-1,) + (1,) * (len(shape) - 1 - dim))
    return loudness


def gaussian(key, shape, scale, bound, pieces=(), held_as=jnp.bfloat16):
    values = scale * jax.random.normal(key, shape, jnp.float32)
    if pieces:
        values = values * steps_of(key, shape, pieces, -0.22, 0.18)
    return jnp.clip(values, -bound, bound).astype(held_as)


def setup_inputs(seed: int = 0) -> dict:
    streams_of = jax.random.split(jax.random.key(seed), 6)
    queries = draw_queries(jax.random.fold_in(streams_of[5], 71), 0)
    keys = draw_keys(jax.random.fold_in(streams_of[5], 71), 0)
    values = draw_values(jax.random.fold_in(streams_of[5], 71), 0)
    beta = jnp.clip(jax.random.uniform(streams_of[3], (HEADS,), jnp.float32, -2.0, 2.0) * steps_of(streams_of[3], (HEADS,), ((0, 4),), -0.4, 0.0), -2.0, 2.0)
    w_out = gaussian(streams_of[4], (HEADS * HD, D), (HEADS * HD) ** -0.5, 0.09375, ((0, 4),))
    return dict(queries=queries, keys=keys, values=values, beta=beta, w_out=w_out)


def elu_plus(inputs):
    return jnp.where(inputs > 0, inputs + 1.0, jnp.exp(jnp.minimum(inputs, 0.0)))


def window_head(packed):
    query_head, key_head, value_head, first_flag = packed
    scores = jnp.dot(query_head, key_head.T, preferred_element_type=jnp.float32) * (HD ** -0.5)
    query_pos = jnp.arange(SEG)[:, None] + SEG
    key_pos = jnp.arange(2 * SEG)[None, :]
    visible = (key_pos <= query_pos) & (key_pos > query_pos - SEG) & ((key_pos >= SEG) | (first_flag < 1))
    scores = jnp.where(visible, scores, -jnp.inf)
    highest = jnp.max(scores, axis=-1, keepdims=True)
    weights = jnp.exp(scores - highest)
    total = jnp.sum(weights, axis=-1, keepdims=True)
    rounded = weights.astype(jnp.bfloat16)
    summed = jnp.dot(rounded, value_head, preferred_element_type=jnp.float32)
    return summed / total


def segment_attention(packed):
    query_seg, key_seg, value_seg, key_prev, value_prev, first_flag = packed
    key_both = jnp.concatenate([key_prev, key_seg], axis=0)
    value_both = jnp.concatenate([value_prev, value_seg], axis=0)
    flags = jnp.full((HEADS,), first_flag, jnp.int32)
    result = lax.map(window_head, (jnp.transpose(query_seg, (1, 0, 2)), jnp.transpose(key_both, (1, 0, 2)), jnp.transpose(value_both, (1, 0, 2)), flags))
    return jnp.transpose(result, (1, 0, 2))


def segment_terms(packed):
    key_seg, value_seg = packed
    soft_keys = elu_plus(key_seg.astype(jnp.float32)).astype(jnp.bfloat16)
    outer = jnp.einsum("thd,the->hde", soft_keys.astype(jnp.float32), value_seg.astype(jnp.float32))
    totals = jnp.sum(soft_keys.astype(jnp.float32), axis=0)
    return outer, totals


def reference(queries, keys, values, beta, w_out):
    segments = TOKENS // SEG
    shaped = (segments, SEG, HEADS, HD)
    query_all = queries.reshape(shaped)
    key_all = keys.reshape(shaped)
    value_all = values.reshape(shaped)
    terms, norms = lax.map(segment_terms, (key_all, value_all))
    memory = jnp.concatenate([jnp.zeros((1, HEADS, HD, HD), jnp.float32), jnp.cumsum(terms, axis=0)[:-1]], axis=0)
    norm_prev = jnp.concatenate([jnp.zeros((1, HEADS, HD), jnp.float32), jnp.cumsum(norms, axis=0)[:-1]], axis=0)
    soft_queries = lax.optimization_barrier(elu_plus(query_all.astype(jnp.float32)).astype(jnp.bfloat16)).astype(jnp.float32)
    numer = jnp.einsum("sthd,shde->sthe", soft_queries, memory, precision=lax.Precision.HIGHEST)
    denom = 1.0 + jnp.einsum("sthd,shd->sth", soft_queries, norm_prev, precision=lax.Precision.HIGHEST)
    from_memory = numer / denom[..., None]
    zero_seg = jnp.zeros((1, SEG, HEADS, HD), jnp.bfloat16)
    key_prev = jnp.concatenate([zero_seg, key_all[:-1]], axis=0)
    value_prev = jnp.concatenate([zero_seg, value_all[:-1]], axis=0)
    first_flags = (jnp.arange(segments) == 0).astype(jnp.int32)
    local = lax.map(segment_attention, (query_all, key_all, value_all, key_prev, value_prev, first_flags))
    gate = jax.nn.sigmoid(beta.astype(jnp.float32))[None, None, :, None]
    attended = (gate * from_memory + (1.0 - gate) * local).astype(jnp.bfloat16).reshape(TOKENS, HEADS * HD)
    return jnp.dot(attended, w_out, preferred_element_type=jnp.float32).astype(jnp.bfloat16)
```

```python
import jax
import jax.numpy as jnp
from jax import lax
from jax.experimental import pallas as pl
from jax.experimental.pallas import tpu as pltpu
from jax.sharding import Mesh
from jax.sharding import PartitionSpec as P

HD = 128
BLK = 256
NB = 8
PLANE = ("seq_1", "seq_2")
SCALE2 = (HD**-0.5) * 1.4426950408889634
F32 = jnp.float32
BF16 = jnp.bfloat16
ANY = pl.BlockSpec(memory_space=pl.ANY)
SMEM = pl.BlockSpec(memory_space=pltpu.SMEM)
VMEM = pl.BlockSpec(memory_space=pltpu.VMEM)


def shifted(block, axis, distance, wrap=True):
    size = lax.axis_size(axis)
    if wrap:
        route = [(i, (i + distance) % size) for i in range(size)]
    else:
        route = [(i, i + distance) for i in range(size - distance)]
    return lax.ppermute(block, axis, route)


def elu_plus(inputs):
    return jnp.where(inputs > 0, inputs + 1.0, jnp.exp(jnp.minimum(inputs, 0.0)))


def slot_of(here, d):
    return lax.rem(here - d + NB, NB)


def params(flops, nbytes):
    return dict(
        cost_estimate=pl.CostEstimate(flops=flops, bytes_accessed=nbytes, transcendentals=0),
        compiler_params=pltpu.CompilerParams(vmem_limit_bytes=48 * 1024 * 1024),
    )


def gather_pieces(here, pieces, buffer, sems, base, pick=None):
    copies = []
    for d, piece in enumerate(pieces):
        source = piece if pick is None else piece.at[pick]
        start = pl.multiple_of(slot_of(here, d) * BLK, BLK)
        copy = pltpu.make_async_copy(source, buffer.at[pl.ds(start, BLK)], sems.at[base + d])
        copy.start()
        copies.append(copy)
    return copies


def terms_kernel(*refs):
    pieces, out, kv, sems = refs[:NB], refs[NB], refs[NB + 1], refs[NB + 2]
    copies = []
    for d in range(NB):
        copy = pltpu.make_async_copy(pieces[d], kv.at[d], sems.at[d])
        copy.start()
        copies.append(copy)
    outer = jnp.zeros((HD, HD), F32)
    totals = jnp.zeros((8, HD), F32)
    for d in range(NB):
        copies[d].wait()
        soft = elu_plus(kv[d, 0].astype(F32)).astype(BF16)
        outer = outer + lax.dot_general(
            soft, kv[d, 1], (((0,), (0,)), ((), ())), preferred_element_type=F32
        )
        totals = totals + jnp.dot(jnp.ones((8, BLK), BF16), soft, preferred_element_type=F32)
    out[0:HD, :] = outer
    out[HD : HD + 8, :] = totals


def memory_terms(pieces):
    return pl.pallas_call(
        terms_kernel,
        out_shape=jax.ShapeDtypeStruct((HD + 8, HD), F32),
        in_specs=[ANY] * NB,
        out_specs=VMEM,
        scratch_shapes=[
            pltpu.VMEM((NB, 2, BLK, HD), BF16),
            pltpu.SemaphoreType.DMA((NB,)),
        ],
        name="terms",
        **params(2 * 2048 * HD * HD, 1 << 20),
    )(*pieces)


def attend(query, keys, values_ones, scores, first, count, mask_at, mask, start_max=None):
    peak = start_max
    for j in range(count):
        rows = pl.ds((first + j) * BLK, BLK)
        part = lax.dot_general(
            query, keys[rows, :], (((1,), (1,)), ((), ())), preferred_element_type=F32
        )
        if j == mask_at:
            part = jnp.where(mask, part, -jnp.inf)
        scores[:, j * BLK : (j + 1) * BLK] = part
        high = jnp.maximum(part[:, :HD], part[:, HD:])
        peak = high if peak is None else jnp.maximum(peak, high)
    peak = jnp.max(peak, axis=1, keepdims=True)
    shift = peak * SCALE2
    acc = None
    for j in range(count):
        rows = pl.ds((first + j) * BLK, BLK)
        weights = jnp.exp2(scores[:, j * BLK : (j + 1) * BLK] * SCALE2 - shift).astype(BF16)
        part = jnp.dot(weights, values_ones[rows, :], preferred_element_type=F32)
        acc = part if acc is None else acc + part
    return acc, peak


def own_kernel(*refs):
    here_ref = refs[0]
    kvs, qs = refs[1 : 1 + NB], refs[1 + NB : 1 + 2 * NB]
    acc_out, peak_out = refs[1 + 2 * NB : 3 + 2 * NB]
    keys, values, query, scores_a, scores_b, sems = refs[3 + 2 * NB :]
    here = here_ref[0]
    copies = gather_pieces(here, qs, query, sems, 0)
    copies += gather_pieces(here, kvs, keys, sems, NB, 0)
    copies += gather_pieces(here, kvs, values.at[:, pl.ds(0, HD)], sems, 2 * NB, 1)
    values[:, HD:] = jnp.ones((NB * BLK, HD), BF16)
    for copy in copies:
        copy.wait()
    row = lax.broadcasted_iota(jnp.int32, (BLK, BLK), 0)
    col = lax.broadcasted_iota(jnp.int32, (BLK, BLK), 1)
    for b in range(NB):
        rows = pl.ds(b * BLK, BLK)
        acc, peak = attend(
            query[rows, :], keys, values, (scores_a, scores_b)[b % 2], 0, b + 1, b, col <= row
        )
        acc_out[rows, :] = acc
        peak_out[rows, :] = jnp.broadcast_to(peak, (BLK, HD))


def own_part(here, kvs, qs):
    rows = NB * BLK
    return pl.pallas_call(
        own_kernel,
        out_shape=(
            jax.ShapeDtypeStruct((rows, 2 * HD), F32),
            jax.ShapeDtypeStruct((rows, HD), F32),
        ),
        in_specs=[SMEM] + [ANY] * (2 * NB),
        out_specs=(VMEM, VMEM),
        scratch_shapes=[
            pltpu.VMEM((rows, HD), BF16),
            pltpu.VMEM((rows, 2 * HD), BF16),
            pltpu.VMEM((rows, HD), BF16),
            pltpu.VMEM((BLK, rows), F32),
            pltpu.VMEM((BLK, rows), F32),
            pltpu.SemaphoreType.DMA((3 * NB,)),
        ],
        name="own",
        **params(36 * BLK * BLK * HD * 8, 5 << 20),
    )(here, *kvs, *qs)


def past_kernel(*refs):
    here_ref, beta_ref = refs[0], refs[1]
    kvs, qs = refs[2 : 2 + NB], refs[2 + NB : 2 + 2 * NB]
    acc_in, peak_in, memory_ref = refs[2 + 2 * NB : 5 + 2 * NB]
    outs = refs[5 + 2 * NB : 5 + 3 * NB]
    keys, values, query, scores_a, scores_b, result, acc_buf, sems = refs[5 + 3 * NB :]
    here, segment = here_ref[0], here_ref[1]
    copies = gather_pieces(here, qs, query, sems, 0)
    copies += gather_pieces(here, kvs, keys, sems, NB, 0)
    copies += gather_pieces(here, kvs, values.at[:, pl.ds(0, HD)], sems, 2 * NB, 1)
    values[:, HD:] = jnp.ones((NB * BLK, HD), BF16)
    for copy in copies:
        copy.wait()

    @pl.when(segment == 0)
    def _():
        acc_buf[...] = acc_in[...]

    @pl.when(segment > 0)
    def _():
        row = lax.broadcasted_iota(jnp.int32, (BLK, BLK), 0)
        col = lax.broadcasted_iota(jnp.int32, (BLK, BLK), 1)
        for b in range(NB):
            rows = pl.ds(b * BLK, BLK)
            before = peak_in[rows, :]
            acc, peak = attend(
                query[rows, :],
                keys,
                values,
                (scores_a, scores_b)[b % 2],
                b,
                NB - b,
                0,
                col > row,
                before,
            )
            fade = jnp.exp2((before - peak) * SCALE2)
            acc_buf[rows, :HD] = acc[:, :HD] + acc_in[rows, :HD] * fade
            acc_buf[rows, HD:] = acc[:, HD:] + acc_in[rows, HD:] * fade

    memory = memory_ref[0:HD, :]
    norm = jnp.transpose(jnp.broadcast_to(memory_ref[HD : HD + 1, :], (HD, HD)))
    whole = jnp.concatenate([memory, norm], axis=1)
    upper = whole.astype(BF16)
    lower = (whole - upper.astype(F32)).astype(BF16)
    split = jnp.concatenate([upper, lower], axis=0)
    gate = 1.0 / (1.0 + jnp.exp(-jnp.full((1, HD), beta_ref[here], F32)))
    for b in range(NB):
        rows = pl.ds(b * BLK, BLK)
        soft = elu_plus(query[rows, :].astype(F32)).astype(BF16)
        both = jnp.dot(jnp.concatenate([soft, soft], axis=1), split, preferred_element_type=F32)
        from_memory = both[:, :HD] / (1.0 + both[:, HD:])
        local = acc_buf[rows, :HD] / acc_buf[rows, HD:]
        result[rows, :] = (gate * from_memory + (1.0 - gate) * local).astype(BF16)
    leaving = []
    for d in range(NB):
        start = pl.multiple_of(slot_of(here, d) * BLK, BLK)
        copy = pltpu.make_async_copy(result.at[pl.ds(start, BLK)], outs[d], sems.at[d])
        copy.start()
        leaving.append(copy)
    for copy in leaving:
        copy.wait()


def past_part(here, beta, kvs, qs, acc, peak, memory):
    rows = NB * BLK
    return pl.pallas_call(
        past_kernel,
        out_shape=[jax.ShapeDtypeStruct((BLK, HD), BF16)] * NB,
        in_specs=[SMEM, SMEM] + [ANY] * (2 * NB) + [VMEM] * 3,
        out_specs=[ANY] * NB,
        scratch_shapes=[
            pltpu.VMEM((rows, HD), BF16),
            pltpu.VMEM((rows, 2 * HD), BF16),
            pltpu.VMEM((rows, HD), BF16),
            pltpu.VMEM((BLK, rows), F32),
            pltpu.VMEM((BLK, rows), F32),
            pltpu.VMEM((rows, HD), BF16),
            pltpu.VMEM((rows, 2 * HD), F32),
            pltpu.SemaphoreType.DMA((3 * NB,)),
        ],
        name="past",
        **params(36 * BLK * BLK * HD * 8, 6 << 20),
    )(here, beta, *kvs, *qs, acc, peak, memory)


def project_kernel(*refs):
    spot_ref = refs[0]
    pieces, weight = refs[1 : 1 + NB], refs[1 + NB]
    out = refs[2 + NB]
    attended, sems = refs[3 + NB :]

    @pl.when(pl.program_id(0) == 0)
    def _():
        copies = []
        for d in range(NB):
            start = pl.multiple_of(lax.rem(spot_ref[0] + d, NB) * HD, HD)
            copy = pltpu.make_async_copy(pieces[d], attended.at[:, pl.ds(start, HD)], sems.at[d])
            copy.start()
            copies.append(copy)
        for copy in copies:
            copy.wait()

    out[...] = jnp.dot(attended[...], weight[...], preferred_element_type=F32).astype(out.dtype)


def project(spot, pieces, weight, dtype):
    width = weight.shape[1] // 4
    steps = 4
    tile = width // steps
    grid_spec = pltpu.PrefetchScalarGridSpec(
        num_scalar_prefetch=1,
        grid=(steps,),
        in_specs=[ANY] * NB
        + [pl.BlockSpec((NB * HD, tile), lambda n, spot: (0, spot[1] * steps + n))],
        out_specs=pl.BlockSpec((BLK, tile), lambda n, spot: (0, n)),
        scratch_shapes=[
            pltpu.VMEM((BLK, NB * HD), BF16),
            pltpu.SemaphoreType.DMA((NB,)),
        ],
    )
    return pl.pallas_call(
        project_kernel,
        grid_spec=grid_spec,
        out_shape=jax.ShapeDtypeStruct((BLK, width), dtype),
        name="project",
        **params(2 * BLK * NB * HD * width, 3 << 20),
    )(spot, *pieces, weight)


def body(queries, keys, values, beta, w_out):
    here = lax.axis_index(PLANE)
    segment = lax.axis_index("seq_0")
    column = lax.axis_index("head")

    def cut(array, d):
        return lax.dynamic_slice_in_dim(array, ((here + d) % NB) * HD, HD, 1)

    kv_here = [
        jnp.stack((cut(keys, d), cut(values, d))) for d in range(NB)
    ]
    q_here = [cut(queries, d) for d in range(NB)]
    kvs = [kv_here[0]] + [shifted(kv_here[d], PLANE, d) for d in range(1, NB)]
    qs = [q_here[0]] + [shifted(q_here[d], PLANE, d) for d in range(1, NB)]
    kvs_past = [shifted(piece, "seq_0", 1, wrap=False) for piece in kvs]

    memory = shifted(memory_terms(kvs), "seq_0", 1, wrap=False)
    memory = memory + shifted(memory, "seq_0", 1, wrap=False)
    memory = memory + shifted(memory, "seq_0", 2, wrap=False)
    memory = memory + shifted(memory, "seq_0", 4, wrap=False)

    place = jnp.stack((here, segment)).astype(jnp.int32)
    acc, peak = own_part(place, kvs, qs)
    attended = past_part(place, beta, kvs_past, qs, acc, peak, memory)
    heads = [attended[0]] + [shifted(attended[d], PLANE, NB - d) for d in range(1, NB)]

    total = None
    for e in (2, 1, 3, 0):
        spot = jnp.stack((here, (column + e) % 4)).astype(jnp.int32)
        part = project(spot, heads, w_out, BF16 if e else F32)
        if e:
            part = shifted(part, "head", e).astype(F32)
        total = part if total is None else total + part
    return total.astype(BF16)


def solution(mesh):
    torus = Mesh(
        mesh.devices.reshape(8, 4, 2, mesh.shape["head"]), ("seq_0", "seq_1", "seq_2", "head")
    )
    seq = ("seq_0", "seq_1", "seq_2")
    return jax.shard_map(
        body,
        mesh=torus,
        in_specs=(P(seq, "head"), P(seq, "head"), P(seq, "head"), P("head"), P("head", None)),
        out_specs=P(seq, "head"),
        check_vma=False,
    )
```

```python
import jax
import jax.numpy as jnp
from jax import lax
from jax.experimental import pallas as pl
from jax.experimental.pallas import tpu as pltpu
from jax.sharding import Mesh
from jax.sharding import PartitionSpec as P

HD = 128
BLK = 256
NB = 8
PLANE = ("seq_1", "seq_2")
SCALE2 = (HD**-0.5) * 1.4426950408889634
F32 = jnp.float32
BF16 = jnp.bfloat16
ANY = pl.BlockSpec(memory_space=pl.ANY)
SMEM = pl.BlockSpec(memory_space=pltpu.SMEM)
VMEM = pl.BlockSpec(memory_space=pltpu.VMEM)


def shifted(block, axis, distance, wrap=True):
    size = lax.axis_size(axis)
    if wrap:
        route = [(i, (i + distance) % size) for i in range(size)]
    else:
        route = [(i, i + distance) for i in range(size - distance)]
    return lax.ppermute(block, axis, route)


def elu_plus(inputs):
    return jnp.where(inputs > 0, inputs + 1.0, jnp.exp(jnp.minimum(inputs, 0.0)))


def slot_of(here, d):
    return lax.rem(here - d + NB, NB)


def params(flops, nbytes):
    return dict(
        cost_estimate=pl.CostEstimate(flops=flops, bytes_accessed=nbytes, transcendentals=0),
        compiler_params=pltpu.CompilerParams(vmem_limit_bytes=32 * 1024 * 1024),
    )


def place_rows(here, d):
    return pl.ds(pl.multiple_of(slot_of(here, d) * BLK, BLK), BLK)


def split_kernel(*refs):
    here_ref, keys, values, queries = refs[:4]
    kvs, qs = refs[4 : 4 + NB], refs[4 + NB : 4 + 2 * NB]
    sems = refs[4 + 2 * NB]
    here = here_ref[0]
    copies = []
    for d in range(NB):
        cols = pl.ds(pl.multiple_of(lax.rem(here + d, NB) * HD, HD), HD)
        copies.append(pltpu.make_async_copy(keys.at[:, cols], kvs[d].at[0], sems.at[0, d]))
        copies.append(pltpu.make_async_copy(values.at[:, cols], kvs[d].at[1], sems.at[1, d]))
    for d in range(NB):
        cols = pl.ds(pl.multiple_of(lax.rem(here + d, NB) * HD, HD), HD)
        copies.append(pltpu.make_async_copy(queries.at[:, cols], qs[d], sems.at[2, d]))
    for copy in copies:
        copy.start()
    for copy in copies:
        copy.wait()


def split_heads(here, keys, values, queries):
    out = pl.pallas_call(
        split_kernel,
        out_shape=[jax.ShapeDtypeStruct((2, BLK, HD), BF16)] * NB
        + [jax.ShapeDtypeStruct((BLK, HD), BF16)] * NB,
        in_specs=[SMEM] + [ANY] * 3,
        out_specs=[VMEM] * (2 * NB),
        scratch_shapes=[pltpu.SemaphoreType.DMA((3, NB))],
        name="split",
        **params(0, 3 << 20),
    )(here, keys, values, queries)
    return out[:NB], out[NB:]


def terms_kernel(*refs):
    pieces, out = refs[:NB], refs[NB]
    outer = jnp.zeros((HD, HD), F32)
    totals = jnp.zeros((8, HD), F32)
    for d in range(NB):
        soft = elu_plus(pieces[d][0].astype(F32)).astype(BF16)
        outer = outer + lax.dot_general(
            soft, pieces[d][1], (((0,), (0,)), ((), ())), preferred_element_type=F32
        )
        totals = totals + jnp.dot(jnp.ones((8, BLK), BF16), soft, preferred_element_type=F32)
    out[0:HD, :] = outer
    out[HD : HD + 8, :] = totals


def memory_terms(pieces):
    return pl.pallas_call(
        terms_kernel,
        out_shape=jax.ShapeDtypeStruct((HD + 8, HD), F32),
        in_specs=[VMEM] * NB,
        out_specs=VMEM,
        name="terms",
        **params(2 * 2048 * HD * HD, 1 << 20),
    )(*pieces)


def attend(query, keys, values_ones, scores, first, count, mask_at, mask, start_max=None):
    peak = start_max
    for j in range(count):
        rows = pl.ds((first + j) * BLK, BLK)
        part = lax.dot_general(
            query, keys[rows, :], (((1,), (1,)), ((), ())), preferred_element_type=F32
        )
        if j == mask_at:
            part = jnp.where(mask, part, -jnp.inf)
        scores[:, j * BLK : (j + 1) * BLK] = part
        high = jnp.maximum(part[:, :HD], part[:, HD:])
        peak = high if peak is None else jnp.maximum(peak, high)
    peak = jnp.max(peak, axis=1, keepdims=True)
    shift = peak * SCALE2
    acc = None
    for j in range(count):
        rows = pl.ds((first + j) * BLK, BLK)
        weights = jnp.exp2(scores[:, j * BLK : (j + 1) * BLK] * SCALE2 - shift).astype(BF16)
        part = jnp.dot(weights, values_ones[rows, :], preferred_element_type=F32)
        acc = part if acc is None else acc + part
    return acc, peak


def own_kernel(*refs):
    here_ref = refs[0]
    kvs, qs = refs[1 : 1 + NB], refs[1 + NB : 1 + 2 * NB]
    weight, acc_out, peak_out, weight_out = refs[1 + 2 * NB : 5 + 2 * NB]
    keys, values, query, scores_a, scores_b, sem = refs[5 + 2 * NB :]
    fetch = pltpu.make_async_copy(weight, weight_out, sem)
    fetch.start()
    here = here_ref[0]
    for d in range(NB):
        rows = place_rows(here, d)
        keys[rows, :] = kvs[d][0]
        values[rows, :HD] = kvs[d][1]
        query[rows, :] = qs[d][...]
    values[:, HD:] = jnp.ones((NB * BLK, HD), BF16)
    row = lax.broadcasted_iota(jnp.int32, (BLK, BLK), 0)
    col = lax.broadcasted_iota(jnp.int32, (BLK, BLK), 1)
    for b in range(NB):
        rows = pl.ds(b * BLK, BLK)
        acc, peak = attend(
            query[rows, :], keys, values, (scores_a, scores_b)[b % 2], 0, b + 1, b, col <= row
        )
        acc_out[rows, :] = acc
        peak_out[rows, :] = jnp.broadcast_to(peak, (BLK, HD))
    fetch.wait()


def own_part(here, kvs, qs, weight):
    rows = NB * BLK
    return pl.pallas_call(
        own_kernel,
        out_shape=(
            jax.ShapeDtypeStruct((rows, 2 * HD), F32),
            jax.ShapeDtypeStruct((rows, HD), F32),
            jax.ShapeDtypeStruct(weight.shape, BF16),
        ),
        in_specs=[SMEM] + [VMEM] * (2 * NB) + [ANY],
        out_specs=(VMEM, VMEM, VMEM),
        scratch_shapes=[
            pltpu.VMEM((rows, HD), BF16),
            pltpu.VMEM((rows, 2 * HD), BF16),
            pltpu.VMEM((rows, HD), BF16),
            pltpu.VMEM((BLK, rows), F32),
            pltpu.VMEM((BLK, rows), F32),
            pltpu.SemaphoreType.DMA,
        ],
        name="own",
        **params(36 * BLK * BLK * HD * 8, 5 << 20),
    )(here, *kvs, *qs, weight)


def past_kernel(*refs):
    here_ref, beta_ref = refs[0], refs[1]
    near, far = refs[2:4]
    qs = refs[4 : 4 + NB]
    acc_in, peak_in, memory_ref, more_ref, less_ref = refs[4 + NB : 9 + NB]
    outs = refs[9 + NB : 9 + 2 * NB]
    keys, values, query, scores_a, scores_b, result, acc_buf = refs[9 + 2 * NB :]
    here, segment = here_ref[0], here_ref[1]
    for d in range(NB):
        rows = place_rows(here, d)
        part = (near, far)[d // 4]
        keys[rows, :] = part[2 * (d % 4)]
        values[rows, :HD] = part[2 * (d % 4) + 1]
        query[rows, :] = qs[d][...]
    values[:, HD:] = jnp.ones((NB * BLK, HD), BF16)

    @pl.when(segment == 0)
    def _():
        acc_buf[...] = acc_in[...]

    @pl.when(segment > 0)
    def _():
        row = lax.broadcasted_iota(jnp.int32, (BLK, BLK), 0)
        col = lax.broadcasted_iota(jnp.int32, (BLK, BLK), 1)
        for b in range(NB):
            rows = pl.ds(b * BLK, BLK)
            before = peak_in[rows, :]
            acc, peak = attend(
                query[rows, :],
                keys,
                values,
                (scores_a, scores_b)[b % 2],
                b,
                NB - b,
                0,
                col > row,
                before,
            )
            fade = jnp.exp2((before - peak) * SCALE2)
            acc_buf[rows, :HD] = acc[:, :HD] + acc_in[rows, :HD] * fade
            acc_buf[rows, HD:] = acc[:, HD:] + acc_in[rows, HD:] * fade

    total = (memory_ref[...] - less_ref[...]) + more_ref[...]
    memory = total[0:HD, :]
    norm = jnp.transpose(jnp.broadcast_to(total[HD : HD + 1, :], (HD, HD)))
    whole = jnp.concatenate([memory, norm], axis=1)
    upper = whole.astype(BF16)
    lower = (whole - upper.astype(F32)).astype(BF16)
    split = jnp.concatenate([upper, lower], axis=0)
    gate = 1.0 / (1.0 + jnp.exp(-jnp.full((1, HD), beta_ref[here], F32)))
    for b in range(NB):
        rows = pl.ds(b * BLK, BLK)
        soft = elu_plus(query[rows, :].astype(F32)).astype(BF16)
        both = jnp.dot(jnp.concatenate([soft, soft], axis=1), split, preferred_element_type=F32)
        from_memory = both[:, :HD] / (1.0 + both[:, HD:])
        local = acc_buf[rows, :HD] / acc_buf[rows, HD:]
        result[rows, :] = (gate * from_memory + (1.0 - gate) * local).astype(BF16)
    for d in range(NB):
        outs[d][...] = result[place_rows(here, d), :]


def past_part(here, beta, kvs, qs, acc, peak, memory):
    rows = NB * BLK
    return pl.pallas_call(
        past_kernel,
        out_shape=[jax.ShapeDtypeStruct((BLK, HD), BF16)] * NB,
        in_specs=[SMEM, SMEM] + [VMEM] * (7 + NB),
        out_specs=[VMEM] * NB,
        scratch_shapes=[
            pltpu.VMEM((rows, HD), BF16),
            pltpu.VMEM((rows, 2 * HD), BF16),
            pltpu.VMEM((rows, HD), BF16),
            pltpu.VMEM((BLK, rows), F32),
            pltpu.VMEM((BLK, rows), F32),
            pltpu.VMEM((rows, HD), BF16),
            pltpu.VMEM((rows, 2 * HD), F32),
        ],
        name="past",
        **params(36 * BLK * BLK * HD * 8, 6 << 20),
    )(here, beta, *kvs, *qs, acc, peak, *memory)


def project_kernel(*refs):
    spot_ref = refs[0]
    pieces, weight = refs[1 : 1 + NB], refs[1 + NB]
    out = refs[2 + NB]
    attended = refs[3 + NB]
    for d in range(NB):
        start = pl.multiple_of(lax.rem(spot_ref[0] + d, NB) * HD, HD)
        attended[:, pl.ds(start, HD)] = pieces[d][...]
    width = out.shape[1]
    cols = pl.ds(pl.multiple_of(lax.rem(spot_ref[2] + spot_ref[3], 4) * width, width), width)
    out[...] = jnp.dot(
        attended[...], weight[:, cols], preferred_element_type=F32
    ).astype(out.dtype)


def project(place, pieces, weight, dtype):
    width = weight.shape[1] // 4
    return pl.pallas_call(
        project_kernel,
        in_specs=[SMEM] + [VMEM] * (1 + NB),
        out_specs=VMEM,
        scratch_shapes=[pltpu.VMEM((BLK, NB * HD), BF16)],
        out_shape=jax.ShapeDtypeStruct((BLK, width), dtype),
        name="project",
        **params(2 * BLK * NB * HD * width, 3 << 20),
    )(place, *pieces, weight)


def body(queries, keys, values, beta, w_out):
    here = lax.axis_index(PLANE)
    segment = lax.axis_index("seq_0")
    column = lax.axis_index("head")

    def place(e):
        return jnp.stack((here, segment, column, e)).astype(jnp.int32)

    kv_here, q_here = split_heads(place(0), keys, values, queries)
    kvs = [kv_here[0]] + [shifted(kv_here[d], PLANE, d) for d in range(1, NB)]
    kvs_past = [
        shifted(jnp.concatenate(kvs[:4]), "seq_0", 1, wrap=False),
        shifted(jnp.concatenate(kvs[4:]), "seq_0", 1, wrap=False),
    ]
    qs = [q_here[0]] + [shifted(q_here[d], PLANE, d) for d in range(1, NB)]

    terms = memory_terms(kvs)
    memory = terms + shifted(terms, "seq_0", 1, wrap=False)
    memory = memory + shifted(memory, "seq_0", 2, wrap=False)
    memory = (memory, shifted(memory, "seq_0", 4, wrap=False), terms)

    acc, peak, weight = own_part(place(0), kvs, qs, w_out)
    attended = past_part(place(0), beta, kvs_past, qs, acc, peak, memory)
    heads = [attended[0]] + [shifted(attended[d], PLANE, NB - d) for d in range(1, NB)]

    total = None
    for e in (2, 1, 3, 0):
        part = project(place(e), heads, weight, BF16 if e else F32)
        if e:
            part = shifted(part, "head", e).astype(F32)
        total = part if total is None else total + part
    return total.astype(BF16)


def solution(mesh):
    torus = Mesh(
        mesh.devices.reshape(8, 4, 2, mesh.shape["head"]), ("seq_0", "seq_1", "seq_2", "head")
    )
    seq = ("seq_0", "seq_1", "seq_2")
    return jax.shard_map(
        body,
        mesh=torus,
        in_specs=(P(seq, "head"), P(seq, "head"), P(seq, "head"), P("head"), P("head", None)),
        out_specs=P(seq, "head"),
        check_vma=False,
    )
```

```python
import jax
import jax.numpy as jnp
from jax import lax
from jax.experimental import pallas as pl
from jax.experimental.pallas import tpu as pltpu
from jax.sharding import Mesh
from jax.sharding import PartitionSpec as P


HD = 128
BLK = 256
NB = 8
PLANE = ("seq_1", "seq_2")
SCALE2 = (HD**-0.5) * 1.4426950408889634
F32 = jnp.float32
BF16 = jnp.bfloat16
ANY = pl.BlockSpec(memory_space=pl.ANY)
SMEM = pl.BlockSpec(memory_space=pltpu.SMEM)
VMEM = pl.BlockSpec(memory_space=pltpu.VMEM)
HBM = pl.BlockSpec(memory_space=pltpu.HBM)
NEAR = (0, 1, 7, 2, 6)
FAR = (3, 5, 4)


def shifted(block, axis, distance, wrap=True):
    size = lax.axis_size(axis)
    if wrap:
        route = [(i, (i + distance) % size) for i in range(size)]
    else:
        route = [(i, i + distance) for i in range(size - distance)]
    return lax.ppermute(block, axis, route)


def elu_plus(inputs):
    return jnp.where(inputs > 0, inputs + 1.0, jnp.exp(jnp.minimum(inputs, 0.0)))


def slot_of(here, d):
    return lax.rem(here - d + NB, NB)


def params(flops, nbytes, room=16):
    return dict(
        cost_estimate=pl.CostEstimate(flops=flops, bytes_accessed=nbytes, transcendentals=0),
        compiler_params=pltpu.CompilerParams(vmem_limit_bytes=room * 1024 * 1024),
    )


def place_rows(here, d):
    return pl.ds(pl.multiple_of(slot_of(here, d) * BLK, BLK), BLK)


def split_kernel(*refs):
    here_ref, keys, values, queries = refs[:4]
    kvs, qs = refs[4 : 4 + NB], refs[4 + NB : 4 + 2 * NB]
    sems = refs[4 + 2 * NB]
    here = here_ref[0]
    copies = []
    for d in range(NB):
        cols = pl.ds(pl.multiple_of(lax.rem(here + d, NB) * HD, HD), HD)
        copies.append(pltpu.make_async_copy(keys.at[:, cols], kvs[d].at[0], sems.at[0, d]))
        copies.append(pltpu.make_async_copy(values.at[:, cols], kvs[d].at[1], sems.at[1, d]))
    for d in range(NB):
        cols = pl.ds(pl.multiple_of(lax.rem(here + d, NB) * HD, HD), HD)
        copies.append(pltpu.make_async_copy(queries.at[:, cols], qs[d], sems.at[2, d]))
    for copy in copies:
        copy.start()
    for copy in copies:
        copy.wait()


def split_heads(here, keys, values, queries):
    out = pl.pallas_call(
        split_kernel,
        out_shape=[jax.ShapeDtypeStruct((2, BLK, HD), BF16)] * NB
        + [jax.ShapeDtypeStruct((BLK, HD), BF16)] * NB,
        in_specs=[SMEM] + [HBM] * 3,
        out_specs=[VMEM] * (2 * NB),
        scratch_shapes=[pltpu.SemaphoreType.DMA((3, NB))],
        name="split",
        **params(0, 3 << 20),
    )(here, keys, values, queries)
    return out[:NB], out[NB:]


def pack_kernel(*refs):
    for spot, piece in enumerate(refs[:-1]):
        refs[-1][2 * spot : 2 * spot + 2] = piece[...]


def pack(pieces):
    return pl.pallas_call(
        pack_kernel,
        out_shape=jax.ShapeDtypeStruct((2 * len(pieces), BLK, HD), BF16),
        in_specs=[VMEM] * len(pieces),
        out_specs=VMEM,
        name="pack",
        **params(0, 1 << 18),
    )(*pieces)


def terms_kernel(*refs):
    pieces, out = refs[:NB], refs[NB]
    outer = jnp.zeros((HD, HD), F32)
    totals = jnp.zeros((8, HD), F32)
    for d in range(NB):
        soft = elu_plus(pieces[d][0].astype(F32)).astype(BF16)
        outer = outer + lax.dot_general(
            soft, pieces[d][1], (((0,), (0,)), ((), ())), preferred_element_type=F32
        )
        totals = totals + jnp.dot(jnp.ones((8, BLK), BF16), soft, preferred_element_type=F32)
    out[0:HD, :] = outer
    out[HD : HD + 8, :] = totals


def memory_terms(pieces):
    return pl.pallas_call(
        terms_kernel,
        out_shape=jax.ShapeDtypeStruct((HD + 8, HD), F32),
        in_specs=[VMEM] * NB,
        out_specs=VMEM,
        name="terms",
        **params(2 * 2048 * HD * HD, 1 << 20),
    )(*pieces)


def attend(query, keys, values_ones, scores, first, count, mask_at, mask, start_max=None):
    peak = start_max
    for j in range(count):
        rows = pl.ds((first + j) * BLK, BLK)
        part = lax.dot_general(
            query, keys[rows, :], (((1,), (1,)), ((), ())), preferred_element_type=F32
        )
        if j == mask_at:
            part = jnp.where(mask, part, -jnp.inf)
        scores[:, j * BLK : (j + 1) * BLK] = part
        high = jnp.maximum(part[:, :HD], part[:, HD:])
        peak = high if peak is None else jnp.maximum(peak, high)
    peak = jnp.max(peak, axis=1, keepdims=True)
    shift = peak * SCALE2
    acc = None
    for j in range(count):
        rows = pl.ds((first + j) * BLK, BLK)
        weights = jnp.exp2(scores[:, j * BLK : (j + 1) * BLK] * SCALE2 - shift).astype(BF16)
        part = jnp.dot(weights, values_ones[rows, :], preferred_element_type=F32)
        acc = part if acc is None else acc + part
    return acc, peak


def own_kernel(*refs):
    here_ref = refs[0]
    kvs, qs = refs[1 : 1 + NB], refs[1 + NB : 1 + 2 * NB]
    weight, acc_out, peak_out, weight_out = refs[1 + 2 * NB : 5 + 2 * NB]
    keys, values, query, scores_a, scores_b, sem = refs[5 + 2 * NB :]
    fetch = pltpu.make_async_copy(weight, weight_out, sem)
    fetch.start()
    here = here_ref[0]
    for d in range(NB):
        rows = place_rows(here, d)
        keys[rows, :] = kvs[d][0]
        values[rows, :HD] = kvs[d][1]
        query[rows, :] = qs[d][...]
    values[:, HD:] = jnp.ones((NB * BLK, HD), BF16)
    row = lax.broadcasted_iota(jnp.int32, (BLK, BLK), 0)
    col = lax.broadcasted_iota(jnp.int32, (BLK, BLK), 1)
    for b in range(NB):
        rows = pl.ds(b * BLK, BLK)
        acc, peak = attend(
            query[rows, :], keys, values, (scores_a, scores_b)[b % 2], 0, b + 1, b, col <= row
        )
        acc_out[rows, :] = acc
        peak_out[rows, :] = jnp.broadcast_to(peak, (BLK, HD))
    fetch.wait()


def own_part(here, kvs, qs, weight):
    rows = NB * BLK
    return pl.pallas_call(
        own_kernel,
        out_shape=(
            jax.ShapeDtypeStruct((rows, 2 * HD), F32),
            jax.ShapeDtypeStruct((rows, HD), F32),
            jax.ShapeDtypeStruct(weight.shape, BF16),
        ),
        in_specs=[SMEM] + [VMEM] * (2 * NB) + [HBM],
        out_specs=(VMEM, VMEM, VMEM),
        scratch_shapes=[
            pltpu.VMEM((rows, HD), BF16),
            pltpu.VMEM((rows, 2 * HD), BF16),
            pltpu.VMEM((rows, HD), BF16),
            pltpu.VMEM((BLK, rows), F32),
            pltpu.VMEM((BLK, rows), F32),
            pltpu.SemaphoreType.DMA,
        ],
        name="own",
        **params(36 * BLK * BLK * HD * 8, 5 << 20, 24),
    )(here, *kvs, *qs, weight)


def past_kernel(*refs):
    here_ref, beta_ref = refs[0], refs[1]
    near, far = refs[2:4]
    qs = refs[4 : 4 + NB]
    acc_in, peak_in, memory_ref, more_ref = refs[4 + NB : 8 + NB]
    outs = refs[8 + NB : 8 + 2 * NB]
    keys, values, query, scores_a, scores_b, result, acc_buf = refs[8 + 2 * NB :]
    here, segment = here_ref[0], here_ref[1]
    for d in range(NB):
        rows = place_rows(here, d)
        part, spot = (near, NEAR.index(d)) if d in NEAR else (far, FAR.index(d))
        keys[rows, :] = part[2 * spot]
        values[rows, :HD] = part[2 * spot + 1]
        query[rows, :] = qs[d][...]
    values[:, HD:] = jnp.ones((NB * BLK, HD), BF16)

    @pl.when(segment == 0)
    def _():
        acc_buf[...] = acc_in[...]

    @pl.when(segment > 0)
    def _():
        row = lax.broadcasted_iota(jnp.int32, (BLK, BLK), 0)
        col = lax.broadcasted_iota(jnp.int32, (BLK, BLK), 1)
        for b in range(NB):
            rows = pl.ds(b * BLK, BLK)
            before = peak_in[rows, :]
            acc, peak = attend(
                query[rows, :],
                keys,
                values,
                (scores_a, scores_b)[b % 2],
                b,
                NB - b,
                0,
                col > row,
                before,
            )
            fade = jnp.exp2((before - peak) * SCALE2)
            acc_buf[rows, :HD] = acc[:, :HD] + acc_in[rows, :HD] * fade
            acc_buf[rows, HD:] = acc[:, HD:] + acc_in[rows, HD:] * fade

    total = memory_ref[...] + more_ref[...]
    memory = total[0:HD, :]
    norm = jnp.transpose(jnp.broadcast_to(total[HD : HD + 1, :], (HD, HD)))
    whole = jnp.concatenate([memory, norm], axis=1)
    upper = whole.astype(BF16)
    lower = (whole - upper.astype(F32)).astype(BF16)
    split = jnp.concatenate([upper, lower], axis=0)
    gate = 1.0 / (1.0 + jnp.exp(-jnp.full((1, HD), beta_ref[here], F32)))
    for b in range(NB):
        rows = pl.ds(b * BLK, BLK)
        soft = elu_plus(query[rows, :].astype(F32)).astype(BF16)
        both = jnp.dot(jnp.concatenate([soft, soft], axis=1), split, preferred_element_type=F32)
        from_memory = both[:, :HD] / (1.0 + both[:, HD:])
        local = acc_buf[rows, :HD] / acc_buf[rows, HD:]
        result[rows, :] = (gate * from_memory + (1.0 - gate) * local).astype(BF16)
    for d in range(NB):
        outs[d][...] = result[place_rows(here, d), :]


def past_part(here, beta, kvs, qs, acc, peak, memory):
    rows = NB * BLK
    return pl.pallas_call(
        past_kernel,
        out_shape=[jax.ShapeDtypeStruct((BLK, HD), BF16)] * NB,
        in_specs=[SMEM, SMEM] + [VMEM] * (6 + NB),
        out_specs=[VMEM] * NB,
        scratch_shapes=[
            pltpu.VMEM((rows, HD), BF16),
            pltpu.VMEM((rows, 2 * HD), BF16),
            pltpu.VMEM((rows, HD), BF16),
            pltpu.VMEM((BLK, rows), F32),
            pltpu.VMEM((BLK, rows), F32),
            pltpu.VMEM((rows, HD), BF16),
            pltpu.VMEM((rows, 2 * HD), F32),
        ],
        name="past",
        **params(36 * BLK * BLK * HD * 8, 6 << 20, 24),
    )(here, beta, *kvs, *qs, acc, peak, *memory)


def project_kernel(*refs):
    spot_ref = refs[0]
    pieces, weight = refs[1 : 1 + NB], refs[1 + NB]
    out = refs[2 + NB]
    attended = refs[3 + NB]
    for d in range(NB):
        start = pl.multiple_of(lax.rem(spot_ref[0] + d, NB) * HD, HD)
        attended[:, pl.ds(start, HD)] = pieces[d][...]
    width = out.shape[1]
    cols = pl.ds(pl.multiple_of(lax.rem(spot_ref[2] + spot_ref[3], 4) * width, width), width)
    out[...] = jnp.dot(
        attended[...], weight[:, cols], preferred_element_type=F32
    ).astype(out.dtype)


def project(place, pieces, weight, dtype):
    width = weight.shape[1] // 4
    return pl.pallas_call(
        project_kernel,
        in_specs=[SMEM] + [VMEM] * (1 + NB),
        out_specs=VMEM,
        scratch_shapes=[pltpu.VMEM((BLK, NB * HD), BF16)],
        out_shape=jax.ShapeDtypeStruct((BLK, width), dtype),
        name="project",
        **params(2 * BLK * NB * HD * width, 3 << 20),
    )(place, *pieces, weight)


def layer(queries, keys, values, beta, w_out):
    here = lax.axis_index(PLANE)
    segment = lax.axis_index("seq_0")
    column = lax.axis_index("head")

    def place(e):
        return jnp.stack((here, segment, column, e)).astype(jnp.int32)

    keys, values, queries, w_out = (
        pltpu.with_memory_space_constraint(part, pltpu.HBM)
        for part in (keys, values, queries, w_out)
    )
    kv_here, q_here = split_heads(place(0), keys, values, queries)
    order = NEAR[1:] + FAR
    kvs, qs = {0: kv_here[0]}, {0: q_here[0]}
    for d in order:
        kvs[d] = shifted(kv_here[d], PLANE, d)
    kvs_past = []
    for part in (NEAR, FAR):
        kvs_past.append(shifted(pack([kvs[d] for d in part]), "seq_0", 1, wrap=False))
    for d in order:
        qs[d] = shifted(q_here[d], PLANE, d)
    kvs, qs = [kvs[d] for d in range(NB)], [qs[d] for d in range(NB)]

    terms = memory_terms(kvs)
    after = shifted(terms, "seq_0", -1)
    whole = terms + after
    wrapped = jnp.where(segment == 7, after, 0.0)
    chosen = jnp.where(segment <= 5, whole, wrapped)
    after = shifted(chosen, "seq_0", -2)
    window = jnp.where(segment <= 3, whole, wrapped) + after
    after = shifted(window, "seq_0", -4)
    memory = (jnp.where(segment <= 3, 0.0, window), after)

    acc, peak, weight = own_part(place(0), kvs, qs, w_out)
    attended = past_part(place(0), beta, kvs_past, qs, acc, peak, memory)
    heads = [attended[0]] + [shifted(attended[d], PLANE, NB - d) for d in range(1, NB)]

    total = None
    for e in (2, 1, 3, 0):
        part = project(place(e), heads, weight, BF16 if e else F32)
        if e:
            part = shifted(part, "head", e).astype(F32)
        total = part if total is None else total + part
    return total.astype(BF16)


def solution(mesh):
    torus = Mesh(
        mesh.devices.reshape(8, 4, 2, mesh.shape["head"]), ("seq_0", "seq_1", "seq_2", "head")
    )
    seq = ("seq_0", "seq_1", "seq_2")
    return jax.shard_map(
        layer,
        mesh=torus,
        in_specs=(P(seq, "head"), P(seq, "head"), P(seq, "head"), P("head"), P("head", None)),
        out_specs=P(seq, "head"),
        check_vma=False,
    )
```

```python
import jax
import jax.numpy as jnp
from jax import lax
from jax.experimental import pallas as pl
from jax.experimental.pallas import tpu as pltpu
from jax.sharding import Mesh
from jax.sharding import PartitionSpec as P


HD = 128
BLK = 256
NB = 8
PLANE = ("seq_1", "seq_2")
SCALE2 = (HD**-0.5) * 1.4426950408889634
F32 = jnp.float32
BF16 = jnp.bfloat16
ANY = pl.BlockSpec(memory_space=pl.ANY)
SMEM = pl.BlockSpec(memory_space=pltpu.SMEM)
VMEM = pl.BlockSpec(memory_space=pltpu.VMEM)
HBM = pl.BlockSpec(memory_space=pltpu.HBM)
NEAR = (0, 1, 7, 2, 6)
FAR = (3, 5, 4)
SPLIT = 6


def shifted(block, axis, distance, wrap=True):
    size = lax.axis_size(axis)
    if wrap:
        route = [(i, (i + distance) % size) for i in range(size)]
    else:
        route = [(i, i + distance) for i in range(size - distance)]
    return lax.ppermute(block, axis, route)


def elu_plus(inputs):
    return jnp.where(inputs > 0, inputs + 1.0, jnp.exp(jnp.minimum(inputs, 0.0)))


def slot_of(here, d):
    return lax.rem(here - d + NB, NB)


def params(flops, nbytes, room=16):
    return dict(
        cost_estimate=pl.CostEstimate(flops=flops, bytes_accessed=nbytes, transcendentals=0),
        compiler_params=pltpu.CompilerParams(vmem_limit_bytes=room * 1024 * 1024),
    )


def place_rows(here, d):
    return pl.ds(pl.multiple_of(slot_of(here, d) * BLK, BLK), BLK)


def split_kernel(*refs):
    here_ref, arrays, pieces = refs[0], refs[1:4], refs[4 : 4 + NB]
    whole, sems = refs[4 + NB :]
    here = here_ref[0]
    copies = [
        pltpu.make_async_copy(array, whole.at[n], sems.at[n]) for n, array in enumerate(arrays)
    ]
    for copy in copies:
        copy.start()
    for n, copy in enumerate(copies):
        copy.wait()
        for d in range(NB):
            cols = pl.ds(pl.multiple_of(lax.rem(here + d, NB) * HD, HD), HD)
            pieces[d][n] = whole[n, :, cols]


def split_heads(here, keys, values, queries):
    return pl.pallas_call(
        split_kernel,
        out_shape=[jax.ShapeDtypeStruct((3, BLK, HD), BF16)] * NB,
        in_specs=[SMEM] + [HBM] * 3,
        out_specs=[VMEM] * NB,
        scratch_shapes=[
            pltpu.VMEM((3, BLK, NB * HD), BF16),
            pltpu.SemaphoreType.DMA((3,)),
        ],
        name="split",
        **params(0, 3 << 20),
    )(here, keys, values, queries)


def pack_kernel(*refs):
    for spot, piece in enumerate(refs[:-1]):
        refs[-1][2 * spot : 2 * spot + 2] = piece[0:2]


def pack(pieces):
    return pl.pallas_call(
        pack_kernel,
        out_shape=jax.ShapeDtypeStruct((2 * len(pieces), BLK, HD), BF16),
        in_specs=[VMEM] * len(pieces),
        out_specs=VMEM,
        name="pack",
        **params(0, 1 << 18),
    )(*pieces)


def terms_kernel(*refs):
    pieces, out = refs[:NB], refs[NB]
    outer = jnp.zeros((HD, HD), F32)
    totals = jnp.zeros((8, HD), F32)
    for d in range(NB):
        soft = elu_plus(pieces[d][0].astype(F32)).astype(BF16)
        outer = outer + lax.dot_general(
            soft, pieces[d][1], (((0,), (0,)), ((), ())), preferred_element_type=F32
        )
        totals = totals + jnp.dot(jnp.ones((8, BLK), BF16), soft, preferred_element_type=F32)
    out[0:HD, :] = outer
    out[HD : HD + 8, :] = totals


def memory_terms(pieces):
    return pl.pallas_call(
        terms_kernel,
        out_shape=jax.ShapeDtypeStruct((HD + 8, HD), F32),
        in_specs=[VMEM] * NB,
        out_specs=VMEM,
        name="terms",
        **params(2 * 2048 * HD * HD, 1 << 20),
    )(*pieces)


def attend(query, keys, values_ones, scores, first, count, mask_at, mask, start_max=None):
    peak = start_max
    for j in range(count):
        rows = pl.ds((first + j) * BLK, BLK)
        part = lax.dot_general(
            query, keys[rows, :], (((1,), (1,)), ((), ())), preferred_element_type=F32
        )
        if j == mask_at:
            part = jnp.where(mask, part, -jnp.inf)
        scores[:, j * BLK : (j + 1) * BLK] = part
        high = jnp.maximum(part[:, :HD], part[:, HD:])
        peak = high if peak is None else jnp.maximum(peak, high)
    peak = jnp.max(peak, axis=1, keepdims=True)
    shift = peak * SCALE2
    acc = None
    for j in range(count):
        rows = pl.ds((first + j) * BLK, BLK)
        weights = jnp.exp2(scores[:, j * BLK : (j + 1) * BLK] * SCALE2 - shift).astype(BF16)
        part = jnp.dot(weights, values_ones[rows, :], preferred_element_type=F32)
        acc = part if acc is None else acc + part
    return acc, peak


def tile_mask():
    row = lax.broadcasted_iota(jnp.int32, (BLK, BLK), 0)
    col = lax.broadcasted_iota(jnp.int32, (BLK, BLK), 1)
    return col <= row


def own_blocks(blocks, query, keys, values, scores, acc_out, peak_out):
    mask = tile_mask()
    for n, b in enumerate(blocks):
        acc, peak = attend(
            query[pl.ds(b * BLK, BLK), :], keys, values, scores[n % 2], 0, b + 1, b, mask
        )
        rows = pl.ds(n * BLK, BLK)
        acc_out[rows, :] = acc
        peak_out[rows, :] = jnp.broadcast_to(peak, (BLK, HD))


def own_first_kernel(*refs):
    here_ref, pieces, weight = refs[0], refs[1 : 1 + NB], refs[1 + NB]
    keys, values, query, acc_out, peak_out, weight_out = refs[2 + NB : 8 + NB]
    scores_a, scores_b, sem = refs[8 + NB :]
    fetch = pltpu.make_async_copy(weight, weight_out, sem)
    fetch.start()
    here = here_ref[0]
    for d in range(NB):
        rows = place_rows(here, d)
        keys[rows, :] = pieces[d][0]
        values[rows, :HD] = pieces[d][1]
        query[rows, :] = pieces[d][2]
    values[:, HD:] = jnp.ones((NB * BLK, HD), BF16)
    own_blocks(range(SPLIT), query, keys, values, (scores_a, scores_b), acc_out, peak_out)
    fetch.wait()


def own_second_kernel(keys, values, query, acc_out, peak_out, scores_a, scores_b):
    own_blocks(range(SPLIT, NB), query, keys, values, (scores_a, scores_b), acc_out, peak_out)


def own_first(here, pieces, weight):
    rows = NB * BLK
    return pl.pallas_call(
        own_first_kernel,
        out_shape=(
            jax.ShapeDtypeStruct((rows, HD), BF16),
            jax.ShapeDtypeStruct((rows, 2 * HD), BF16),
            jax.ShapeDtypeStruct((rows, HD), BF16),
            jax.ShapeDtypeStruct((SPLIT * BLK, 2 * HD), F32),
            jax.ShapeDtypeStruct((SPLIT * BLK, HD), F32),
            jax.ShapeDtypeStruct(weight.shape, BF16),
        ),
        in_specs=[SMEM] + [VMEM] * NB + [HBM],
        out_specs=(VMEM,) * 6,
        scratch_shapes=[
            pltpu.VMEM((BLK, SPLIT * BLK), F32),
            pltpu.VMEM((BLK, SPLIT * BLK), F32),
            pltpu.SemaphoreType.DMA,
        ],
        name="own_first",
        **params(21 * BLK * BLK * HD * 8, 5 << 20),
    )(here, *pieces, weight)


def own_second(keys, values, query):
    rows = NB * BLK
    return pl.pallas_call(
        own_second_kernel,
        out_shape=(
            jax.ShapeDtypeStruct((rows - SPLIT * BLK, 2 * HD), F32),
            jax.ShapeDtypeStruct((rows - SPLIT * BLK, HD), F32),
        ),
        in_specs=[VMEM] * 3,
        out_specs=(VMEM, VMEM),
        scratch_shapes=[pltpu.VMEM((BLK, rows), F32)] * 2,
        name="own_second",
        **params(15 * BLK * BLK * HD * 8, 3 << 20),
    )(keys, values, query)


def prefix_kernel(place_ref, terms, after, chosen, kept):
    segment = place_ref[1]
    whole = terms[...] + after[...]
    wrapped = jnp.where(segment == 7, after[...], 0.0)
    chosen[...] = jnp.where(segment <= 5, whole, wrapped)
    kept[...] = jnp.where(segment <= 3, whole, wrapped)


def prefix_step(place, terms, after):
    shape = jax.ShapeDtypeStruct(terms.shape, F32)
    return pl.pallas_call(
        prefix_kernel,
        out_shape=(shape, shape),
        in_specs=[SMEM, VMEM, VMEM],
        out_specs=(VMEM, VMEM),
        name="prefix",
        **params(0, 1 << 18),
    )(place, terms, after)


def add_kernel(left, right, out):
    out[...] = (left[...] + right[...].astype(F32)).astype(out.dtype)


def added(left, right, dtype):
    return pl.pallas_call(
        add_kernel,
        out_shape=jax.ShapeDtypeStruct(left.shape, dtype),
        in_specs=[VMEM, VMEM],
        out_specs=VMEM,
        name="added",
        **params(0, 1 << 18),
    )(left, right)


def past_kernel(*refs):
    here_ref, beta_ref, near, far, query = refs[:5]
    acc_a, peak_a, acc_b, peak_b, memory_ref, more_ref = refs[5:11]
    outs = refs[11 : 11 + NB]
    keys, values, scores_a, scores_b, result, acc_buf = refs[11 + NB :]
    here, segment = here_ref[0], here_ref[1]

    def own(b):
        if b < SPLIT:
            rows = pl.ds(b * BLK, BLK)
            return acc_a, peak_a, rows
        return acc_b, peak_b, pl.ds((b - SPLIT) * BLK, BLK)

    @pl.when(segment == 0)
    def _():
        acc_buf[: SPLIT * BLK, :] = acc_a[...]
        acc_buf[SPLIT * BLK :, :] = acc_b[...]

    @pl.when(segment > 0)
    def _():
        for d in range(NB):
            rows = place_rows(here, d)
            part, spot = (near, NEAR.index(d)) if d in NEAR else (far, FAR.index(d))
            keys[rows, :] = part[2 * spot]
            values[rows, :HD] = part[2 * spot + 1]
        values[:, HD:] = jnp.ones((NB * BLK, HD), BF16)
        mask = jnp.logical_not(tile_mask())
        for b in range(NB):
            rows = pl.ds(b * BLK, BLK)
            acc_in, peak_in, own_rows = own(b)
            before = peak_in[own_rows, :]
            acc, peak = attend(
                query[rows, :],
                keys,
                values,
                (scores_a, scores_b)[b % 2],
                b,
                NB - b,
                0,
                mask,
                before,
            )
            fade = jnp.exp2((before - peak) * SCALE2)
            acc_buf[rows, :HD] = acc[:, :HD] + acc_in[own_rows, :HD] * fade
            acc_buf[rows, HD:] = acc[:, HD:] + acc_in[own_rows, HD:] * fade

    total = jnp.where(segment <= 3, 0.0, memory_ref[...]) + more_ref[...]
    memory = total[0:HD, :]
    norm = jnp.transpose(jnp.broadcast_to(total[HD : HD + 1, :], (HD, HD)))
    whole = jnp.concatenate([memory, norm], axis=1)
    upper = whole.astype(BF16)
    lower = (whole - upper.astype(F32)).astype(BF16)
    split = jnp.concatenate([upper, lower], axis=0)
    gate = 1.0 / (1.0 + jnp.exp(-jnp.full((1, HD), beta_ref[here], F32)))
    for b in range(NB):
        rows = pl.ds(b * BLK, BLK)
        soft = elu_plus(query[rows, :].astype(F32)).astype(BF16)
        both = jnp.dot(jnp.concatenate([soft, soft], axis=1), split, preferred_element_type=F32)
        from_memory = both[:, :HD] / (1.0 + both[:, HD:])
        local = acc_buf[rows, :HD] / acc_buf[rows, HD:]
        result[rows, :] = (gate * from_memory + (1.0 - gate) * local).astype(BF16)
    for d in range(NB):
        outs[d][...] = result[place_rows(here, d), :]


def past_part(here, beta, kvs, query, own, memory):
    rows = NB * BLK
    return pl.pallas_call(
        past_kernel,
        out_shape=[jax.ShapeDtypeStruct((BLK, HD), BF16)] * NB,
        in_specs=[SMEM, SMEM] + [VMEM] * 9,
        out_specs=[VMEM] * NB,
        scratch_shapes=[
            pltpu.VMEM((rows, HD), BF16),
            pltpu.VMEM((rows, 2 * HD), BF16),
            pltpu.VMEM((BLK, rows), F32),
            pltpu.VMEM((BLK, rows), F32),
            pltpu.VMEM((rows, HD), BF16),
            pltpu.VMEM((rows, 2 * HD), F32),
        ],
        name="past",
        **params(36 * BLK * BLK * HD * 8, 6 << 20),
    )(here, beta, *kvs, query, *own, *memory)


def project_kernel(*refs):
    spot_ref = refs[0]
    pieces, weight = refs[1 : 1 + NB], refs[1 + NB]
    upper, lower = refs[2 + NB : 4 + NB]
    attended = refs[4 + NB]
    for d in range(NB):
        start = pl.multiple_of(lax.rem(spot_ref[0] + d, NB) * HD, HD)
        attended[:, pl.ds(start, HD)] = pieces[d][...]
    width = upper.shape[1]
    cols = pl.ds(pl.multiple_of(lax.rem(spot_ref[2] + spot_ref[3], 4) * width, width), width)
    whole = jnp.dot(attended[...], weight[:, cols], preferred_element_type=F32)
    upper[...] = whole[: BLK // 2].astype(upper.dtype)
    lower[...] = whole[BLK // 2 :].astype(lower.dtype)


def project(place, pieces, weight, upper, lower):
    width = weight.shape[1] // 4
    return pl.pallas_call(
        project_kernel,
        in_specs=[SMEM] + [VMEM] * (1 + NB),
        out_specs=(VMEM, VMEM),
        scratch_shapes=[pltpu.VMEM((BLK, NB * HD), BF16)],
        out_shape=(
            jax.ShapeDtypeStruct((BLK // 2, width), upper),
            jax.ShapeDtypeStruct((BLK // 2, width), lower),
        ),
        name="project",
        **params(2 * BLK * NB * HD * width, 3 << 20),
    )(place, *pieces, weight)


def finish_kernel(own_up, own_low, up_a, up_b, low_a, low_b, out):
    half = BLK // 2
    out[:half] = (own_up[...] + up_a[...].astype(F32) + up_b[...].astype(F32)).astype(BF16)
    out[half:] = (own_low[...] + low_a[...].astype(F32) + low_b[...].astype(F32)).astype(BF16)


def finish(*parts):
    return pl.pallas_call(
        finish_kernel,
        in_specs=[VMEM] * 6,
        out_specs=VMEM,
        out_shape=jax.ShapeDtypeStruct((BLK, parts[0].shape[1]), BF16),
        name="finish",
        **params(0, 3 << 20),
    )(*parts)


def layer(queries, keys, values, beta, w_out):
    here = lax.axis_index(PLANE)
    segment = lax.axis_index("seq_0")
    column = lax.axis_index("head")

    def place(e):
        return jnp.stack((here, segment, column, e)).astype(jnp.int32)

    keys, values, queries, w_out = (
        pltpu.with_memory_space_constraint(part, pltpu.HBM)
        for part in (keys, values, queries, w_out)
    )
    sent = split_heads(place(0), keys, values, queries)
    pieces = {0: sent[0]}
    for d in NEAR[1:] + FAR:
        pieces[d] = shifted(sent[d], PLANE, d)
    kvs_past = []
    for part in (NEAR, FAR):
        kvs_past.append(shifted(pack([pieces[d] for d in part]), "seq_0", 1, wrap=False))
    pieces = [pieces[d] for d in range(NB)]

    terms = memory_terms(pieces)
    after = shifted(terms, "seq_0", -1)
    chosen, kept = prefix_step(place(0), terms, after)
    after = shifted(chosen, "seq_0", -2)
    window = added(kept, after, F32)
    after = shifted(window, "seq_0", -4)

    k_all, v_all, q_all, acc_a, peak_a, weight = own_first(place(0), pieces, w_out)
    acc_b, peak_b = own_second(k_all, v_all, q_all)
    own = (acc_a, peak_a, acc_b, peak_b)
    attended = past_part(place(0), beta, kvs_past, q_all, own, (window, after))
    heads = [attended[0]] + [shifted(attended[d], PLANE, NB - d) for d in range(1, NB)]

    def send(part, distance):
        return shifted(part, "head", distance)

    far_up, far_low = project(place(2), heads, weight, BF16, BF16)
    far_up, far_low = send(far_up, 1), send(far_low, -1)
    right_up, right_low = project(place(1), heads, weight, F32, BF16)
    got_low = send(right_low, 1)
    left_up, left_low = project(place(3), heads, weight, BF16, F32)
    got_up = send(left_up, -1)
    more_up = send(added(right_up, far_up, BF16), 1)
    more_low = send(added(left_low, far_low, BF16), -1)
    own_up, own_low = project(place(0), heads, weight, F32, F32)
    return finish(own_up, own_low, got_up, more_up, got_low, more_low)


def solution(mesh):
    torus = Mesh(
        mesh.devices.reshape(8, 4, 2, mesh.shape["head"]), ("seq_0", "seq_1", "seq_2", "head")
    )
    seq = ("seq_0", "seq_1", "seq_2")
    return jax.shard_map(
        layer,
        mesh=torus,
        in_specs=(P(seq, "head"), P(seq, "head"), P(seq, "head"), P("head"), P("head", None)),
        out_specs=P(seq, "head"),
        check_vma=False,
    )
```

```python
import jax
import jax.numpy as jnp
from jax import lax
from jax.experimental import pallas as pl
from jax.experimental.pallas import tpu as pltpu
from jax.sharding import Mesh
from jax.sharding import PartitionSpec as P


HD = 128
BLK = 256
NB = 8
PLANE = ("seq_1", "seq_2")
SCALE2 = (HD**-0.5) * 1.4426950408889634
F32 = jnp.float32
BF16 = jnp.bfloat16
ANY = pl.BlockSpec(memory_space=pl.ANY)
SMEM = pl.BlockSpec(memory_space=pltpu.SMEM)
VMEM = pl.BlockSpec(memory_space=pltpu.VMEM)
HBM = pl.BlockSpec(memory_space=pltpu.HBM)
NY = 4
PAIR = 2 * BLK
STEPS = (1, 3, 2)
LEAVE = (4, 3, 5, 2, 6, 1, 7)
SPLIT = 6


def shifted(block, axis, distance, wrap=True):
    size = lax.axis_size(axis)
    if wrap:
        route = [(i, (i + distance) % size) for i in range(size)]
    else:
        route = [(i, i + distance) for i in range(size - distance)]
    return lax.ppermute(block, axis, route)


def elu_plus(inputs):
    return jnp.where(inputs > 0, inputs + 1.0, jnp.exp(jnp.minimum(inputs, 0.0)))


def slot_of(here, d):
    return lax.rem(here - d + NB, NB)


def pair_rows(here, step, half):
    row = lax.rem(here // 2 - step + NY, NY) * PAIR + half * BLK
    return pl.ds(pl.multiple_of(row, BLK), BLK)


def params(flops, nbytes, room=16):
    return dict(
        cost_estimate=pl.CostEstimate(flops=flops, bytes_accessed=nbytes, transcendentals=0),
        compiler_params=pltpu.CompilerParams(vmem_limit_bytes=room * 1024 * 1024),
    )


def place_rows(here, d):
    return pl.ds(pl.multiple_of(slot_of(here, d) * BLK, BLK), BLK)


def split_kernel(here_ref, keys, values, queries, stay, leave, whole, sems):
    here = here_ref[0]
    copies = [
        pltpu.make_async_copy(array, whole.at[n], sems.at[n])
        for n, array in enumerate((keys, values, queries))
    ]
    for copy in copies:
        copy.start()
    own_core = lax.rem(here, 2)
    for n, copy in enumerate(copies):
        copy.wait()
        for step in range(NY):
            pair = lax.rem(here // 2 + step, NY) * 2
            for out, core in ((leave, 1 - own_core), (stay, own_core)):
                cols = pl.ds(pl.multiple_of((pair + core) * HD, HD), HD)
                out[step, n] = whole[n, :, cols]


def split_heads(here, keys, values, queries):
    half = jax.ShapeDtypeStruct((NY, 3, BLK, HD), BF16)
    return pl.pallas_call(
        split_kernel,
        out_shape=(half, half),
        in_specs=[SMEM] + [HBM] * 3,
        out_specs=(VMEM, VMEM),
        scratch_shapes=[
            pltpu.VMEM((3, BLK, NB * HD), BF16),
            pltpu.SemaphoreType.DMA((3,)),
        ],
        name="split",
        **params(0, 3 << 20),
    )(here, keys, values, queries)


def pair_kernel(*refs):
    here_ref, stay, got = refs[:3]
    kvs, qs = refs[3 : 3 + NY], refs[3 + NY : 3 + 2 * NY]
    core = lax.rem(here_ref[0], 2)
    for step in range(NY):
        for part, half in ((stay, core), (got, 1 - core)):
            kvs[step][half] = part[step, 0:2]
            qs[step][half] = part[step, 2]


def pair_up(here, stay, got):
    out = pl.pallas_call(
        pair_kernel,
        out_shape=[jax.ShapeDtypeStruct((2, 2, BLK, HD), BF16)] * NY
        + [jax.ShapeDtypeStruct((2, BLK, HD), BF16)] * NY,
        in_specs=[SMEM, VMEM, VMEM],
        out_specs=[VMEM] * (2 * NY),
        name="pair_up",
        **params(0, 3 << 20),
    )(here, stay, got)
    return out[:NY], out[NY:]


def pack_kernel(first, second, out):
    out[0] = first[...]
    out[1] = second[...]


def pack(first, second):
    return pl.pallas_call(
        pack_kernel,
        out_shape=jax.ShapeDtypeStruct((2, *first.shape), BF16),
        in_specs=[VMEM, VMEM],
        out_specs=VMEM,
        name="pack",
        **params(0, 1 << 20),
    )(first, second)


def terms_kernel(*refs):
    pieces, out, wire = refs[:NY], refs[NY], refs[NY + 1]
    outer = jnp.zeros((HD, HD), F32)
    totals = jnp.zeros((8, HD), F32)
    for piece in pieces:
        for half in range(2):
            soft = elu_plus(piece[half, 0].astype(F32)).astype(BF16)
            outer = outer + lax.dot_general(
                soft, piece[half, 1], (((0,), (0,)), ((), ())), preferred_element_type=F32
            )
            totals = totals + jnp.dot(jnp.ones((8, BLK), BF16), soft, preferred_element_type=F32)
    out[0:HD, :] = outer
    out[HD : HD + 8, :] = totals
    wire[0:HD, :] = outer.astype(BF16)
    wire[HD : HD + 8, :] = totals.astype(BF16)


def memory_terms(pieces):
    return pl.pallas_call(
        terms_kernel,
        out_shape=(
            jax.ShapeDtypeStruct((HD + 8, HD), F32),
            jax.ShapeDtypeStruct((HD + 8, HD), BF16),
        ),
        in_specs=[VMEM] * NY,
        out_specs=(VMEM, VMEM),
        name="terms",
        **params(2 * 2048 * HD * HD, 1 << 20),
    )(*pieces)


def attend(query, keys, values_ones, scores, first, count, mask_at, mask, start_max=None):
    peak = start_max
    for j in range(count):
        rows = pl.ds((first + j) * BLK, BLK)
        part = lax.dot_general(
            query, keys[rows, :], (((1,), (1,)), ((), ())), preferred_element_type=F32
        )
        if j == mask_at:
            part = jnp.where(mask, part, -jnp.inf)
        scores[:, j * BLK : (j + 1) * BLK] = part
        high = jnp.maximum(part[:, :HD], part[:, HD:])
        peak = high if peak is None else jnp.maximum(peak, high)
    peak = jnp.max(peak, axis=1, keepdims=True)
    shift = peak * SCALE2
    acc = None
    for j in range(count):
        rows = pl.ds((first + j) * BLK, BLK)
        weights = jnp.exp2(scores[:, j * BLK : (j + 1) * BLK] * SCALE2 - shift).astype(BF16)
        part = jnp.dot(weights, values_ones[rows, :], preferred_element_type=F32)
        acc = part if acc is None else acc + part
    return acc, peak


def tile_mask():
    row = lax.broadcasted_iota(jnp.int32, (BLK, BLK), 0)
    col = lax.broadcasted_iota(jnp.int32, (BLK, BLK), 1)
    return col <= row


def own_blocks(blocks, query, keys, values, scores, acc_out, peak_out):
    mask = tile_mask()
    for n, b in enumerate(blocks):
        acc, peak = attend(
            query[pl.ds(b * BLK, BLK), :], keys, values, scores[n % 2], 0, b + 1, b, mask
        )
        rows = pl.ds(n * BLK, BLK)
        acc_out[rows, :] = acc
        peak_out[rows, :] = jnp.broadcast_to(peak, (BLK, HD))


def own_first_kernel(*refs):
    here_ref, kvs, qs = refs[0], refs[1 : 1 + NY], refs[1 + NY : 1 + 2 * NY]
    weight, keys, values, query, acc_out, peak_out, weight_out = refs[1 + 2 * NY : 8 + 2 * NY]
    scores_a, scores_b, sem = refs[8 + 2 * NY :]
    fetch = pltpu.make_async_copy(weight, weight_out, sem)
    fetch.start()
    here = here_ref[0]
    for step in range(NY):
        for half in range(2):
            rows = pair_rows(here, step, half)
            keys[rows, :] = kvs[step][half, 0]
            values[rows, :HD] = kvs[step][half, 1]
            query[rows, :] = qs[step][half]
    values[:, HD:] = jnp.ones((NB * BLK, HD), BF16)
    own_blocks(range(SPLIT), query, keys, values, (scores_a, scores_b), acc_out, peak_out)
    fetch.wait()


def own_second_kernel(keys, values, query, acc_out, peak_out, scores_a, scores_b):
    own_blocks(range(SPLIT, NB), query, keys, values, (scores_a, scores_b), acc_out, peak_out)


def own_first(here, kvs, qs, weight):
    rows = NB * BLK
    return pl.pallas_call(
        own_first_kernel,
        out_shape=(
            jax.ShapeDtypeStruct((rows, HD), BF16),
            jax.ShapeDtypeStruct((rows, 2 * HD), BF16),
            jax.ShapeDtypeStruct((rows, HD), BF16),
            jax.ShapeDtypeStruct((SPLIT * BLK, 2 * HD), F32),
            jax.ShapeDtypeStruct((SPLIT * BLK, HD), F32),
            jax.ShapeDtypeStruct(weight.shape, BF16),
        ),
        in_specs=[SMEM] + [VMEM] * (2 * NY) + [HBM],
        out_specs=(VMEM,) * 6,
        scratch_shapes=[
            pltpu.VMEM((BLK, SPLIT * BLK), F32),
            pltpu.VMEM((BLK, SPLIT * BLK), F32),
            pltpu.SemaphoreType.DMA,
        ],
        name="own_first",
        **params(21 * BLK * BLK * HD * 8, 5 << 20),
    )(here, *kvs, *qs, weight)


def own_second(keys, values, query):
    rows = NB * BLK
    return pl.pallas_call(
        own_second_kernel,
        out_shape=(
            jax.ShapeDtypeStruct((rows - SPLIT * BLK, 2 * HD), F32),
            jax.ShapeDtypeStruct((rows - SPLIT * BLK, HD), F32),
        ),
        in_specs=[VMEM] * 3,
        out_specs=(VMEM, VMEM),
        scratch_shapes=[pltpu.VMEM((BLK, rows), F32)] * 2,
        name="own_second",
        **params(15 * BLK * BLK * HD * 8, 3 << 20),
    )(keys, values, query)


def prefix_kernel(place_ref, terms, after, chosen, kept):
    segment = place_ref[1]
    passed = after[...].astype(F32)
    whole = terms[...] + passed
    wrapped = jnp.where(segment == 7, passed, 0.0)
    chosen[...] = jnp.where(segment <= 5, whole, wrapped).astype(BF16)
    kept[...] = jnp.where(segment <= 3, whole, wrapped)


def prefix_step(place, terms, after):
    shape = jax.ShapeDtypeStruct(terms.shape, F32)
    return pl.pallas_call(
        prefix_kernel,
        out_shape=(jax.ShapeDtypeStruct(terms.shape, BF16), shape),
        in_specs=[SMEM, VMEM, VMEM],
        out_specs=(VMEM, VMEM),
        name="prefix",
        **params(0, 1 << 18),
    )(place, terms, after)


def window_kernel(kept, after, out, wire):
    out[...] = kept[...] + after[...].astype(F32)
    wire[...] = out[...].astype(BF16)


def window_step(kept, after):
    return pl.pallas_call(
        window_kernel,
        out_shape=(
            jax.ShapeDtypeStruct(kept.shape, F32),
            jax.ShapeDtypeStruct(kept.shape, BF16),
        ),
        in_specs=[VMEM, VMEM],
        out_specs=(VMEM, VMEM),
        name="window",
        **params(0, 1 << 18),
    )(kept, after)


def add_kernel(left, right, out):
    out[...] = (left[...] + right[...].astype(F32)).astype(out.dtype)


def added(left, right, dtype):
    return pl.pallas_call(
        add_kernel,
        out_shape=jax.ShapeDtypeStruct(left.shape, dtype),
        in_specs=[VMEM, VMEM],
        out_specs=VMEM,
        name="added",
        **params(0, 1 << 18),
    )(left, right)


def past_kernel(*refs):
    here_ref, beta_ref, same, near, far, query = refs[:6]
    acc_a, peak_a, acc_b, peak_b, memory_ref, more_ref = refs[6:12]
    outs = refs[12 : 12 + NB]
    keys, values, scores_a, scores_b, result, acc_buf = refs[12 + NB :]
    here, segment = here_ref[0], here_ref[1]

    def own(b):
        if b < SPLIT:
            rows = pl.ds(b * BLK, BLK)
            return acc_a, peak_a, rows
        return acc_b, peak_b, pl.ds((b - SPLIT) * BLK, BLK)

    @pl.when(segment == 0)
    def _():
        acc_buf[: SPLIT * BLK, :] = acc_a[...]
        acc_buf[SPLIT * BLK :, :] = acc_b[...]

    @pl.when(segment > 0)
    def _():
        for step, part in ((0, same), (1, near.at[0]), (3, near.at[1]), (2, far)):
            for half in range(2):
                rows = pair_rows(here, step, half)
                keys[rows, :] = part[half, 0]
                values[rows, :HD] = part[half, 1]
        values[:, HD:] = jnp.ones((NB * BLK, HD), BF16)
        mask = jnp.logical_not(tile_mask())
        for b in range(NB):
            rows = pl.ds(b * BLK, BLK)
            acc_in, peak_in, own_rows = own(b)
            before = peak_in[own_rows, :]
            acc, peak = attend(
                query[rows, :],
                keys,
                values,
                (scores_a, scores_b)[b % 2],
                b,
                NB - b,
                0,
                mask,
                before,
            )
            fade = jnp.exp2((before - peak) * SCALE2)
            acc_buf[rows, :HD] = acc[:, :HD] + acc_in[own_rows, :HD] * fade
            acc_buf[rows, HD:] = acc[:, HD:] + acc_in[own_rows, HD:] * fade

    total = jnp.where(segment <= 3, 0.0, memory_ref[...]) + more_ref[...].astype(F32)
    memory = total[0:HD, :]
    norm = jnp.transpose(jnp.broadcast_to(total[HD : HD + 1, :], (HD, HD)))
    whole = jnp.concatenate([memory, norm], axis=1)
    upper = whole.astype(BF16)
    lower = (whole - upper.astype(F32)).astype(BF16)
    split = jnp.concatenate([upper, lower], axis=0)
    gate = 1.0 / (1.0 + jnp.exp(-jnp.full((1, HD), beta_ref[here], F32)))
    for b in range(NB):
        rows = pl.ds(b * BLK, BLK)
        soft = elu_plus(query[rows, :].astype(F32)).astype(BF16)
        both = jnp.dot(jnp.concatenate([soft, soft], axis=1), split, preferred_element_type=F32)
        from_memory = both[:, :HD] / (1.0 + both[:, HD:])
        local = acc_buf[rows, :HD] / acc_buf[rows, HD:]
        result[rows, :] = (gate * from_memory + (1.0 - gate) * local).astype(BF16)
    for d in range(NB):
        outs[d][...] = result[place_rows(here, d), :]


def past_part(here, beta, kvs, query, own, memory):
    rows = NB * BLK
    return pl.pallas_call(
        past_kernel,
        out_shape=[jax.ShapeDtypeStruct((BLK, HD), BF16)] * NB,
        in_specs=[SMEM, SMEM] + [VMEM] * 10,
        out_specs=[VMEM] * NB,
        scratch_shapes=[
            pltpu.VMEM((rows, HD), BF16),
            pltpu.VMEM((rows, 2 * HD), BF16),
            pltpu.VMEM((BLK, rows), F32),
            pltpu.VMEM((BLK, rows), F32),
            pltpu.VMEM((rows, HD), BF16),
            pltpu.VMEM((rows, 2 * HD), F32),
        ],
        name="past",
        **params(36 * BLK * BLK * HD * 8, 6 << 20),
    )(here, beta, *kvs, query, *own, *memory)


def project_kernel(*refs):
    spot_ref = refs[0]
    pieces, weight = refs[1 : 1 + NB], refs[1 + NB]
    upper, lower = refs[2 + NB : 4 + NB]
    attended = refs[4 + NB]
    for d in range(NB):
        start = pl.multiple_of(lax.rem(spot_ref[0] + d, NB) * HD, HD)
        attended[:, pl.ds(start, HD)] = pieces[d][...]
    width = upper.shape[1]
    cols = pl.ds(pl.multiple_of(lax.rem(spot_ref[2] + spot_ref[3], 4) * width, width), width)
    whole = jnp.dot(attended[...], weight[:, cols], preferred_element_type=F32)
    upper[...] = whole[: BLK // 2].astype(upper.dtype)
    lower[...] = whole[BLK // 2 :].astype(lower.dtype)


def project(place, pieces, weight, upper, lower):
    width = weight.shape[1] // 4
    return pl.pallas_call(
        project_kernel,
        in_specs=[SMEM] + [VMEM] * (1 + NB),
        out_specs=(VMEM, VMEM),
        scratch_shapes=[pltpu.VMEM((BLK, NB * HD), BF16)],
        out_shape=(
            jax.ShapeDtypeStruct((BLK // 2, width), upper),
            jax.ShapeDtypeStruct((BLK // 2, width), lower),
        ),
        name="project",
        **params(2 * BLK * NB * HD * width, 3 << 20),
    )(place, *pieces, weight)


def finish_kernel(own_up, own_low, up_a, up_b, low_a, low_b, out):
    half = BLK // 2
    out[:half] = (own_up[...] + up_a[...].astype(F32) + up_b[...].astype(F32)).astype(BF16)
    out[half:] = (own_low[...] + low_a[...].astype(F32) + low_b[...].astype(F32)).astype(BF16)


def finish(*parts):
    return pl.pallas_call(
        finish_kernel,
        in_specs=[VMEM] * 6,
        out_specs=VMEM,
        out_shape=jax.ShapeDtypeStruct((BLK, parts[0].shape[1]), BF16),
        name="finish",
        **params(0, 3 << 20),
    )(*parts)


def layer(queries, keys, values, beta, w_out):
    here = lax.axis_index(PLANE)
    segment = lax.axis_index("seq_0")
    column = lax.axis_index("head")

    def place(e):
        return jnp.stack((here, segment, column, e)).astype(jnp.int32)

    keys, values, queries, w_out = (
        pltpu.with_memory_space_constraint(part, pltpu.HBM)
        for part in (keys, values, queries, w_out)
    )
    stay, leave = split_heads(place(0), keys, values, queries)
    got = shifted(leave, "seq_2", 1)
    kvs, qs = map(list, pair_up(place(0), stay, got))
    past = [shifted(kvs[0], "seq_0", 1)]
    for step in STEPS:
        kvs[step] = shifted(kvs[step], "seq_1", step)
    past.append(shifted(pack(kvs[1], kvs[3]), "seq_0", 1))
    past.append(shifted(kvs[2], "seq_0", 1))
    for step in STEPS:
        qs[step] = shifted(qs[step], "seq_1", step)

    terms, wire = memory_terms(kvs)
    after = shifted(wire, "seq_0", -1)
    chosen, kept = prefix_step(place(0), terms, after)
    after = shifted(chosen, "seq_0", -2)
    window, wire = window_step(kept, after)
    after = shifted(wire, "seq_0", -4)

    k_all, v_all, q_all, acc_a, peak_a, weight = own_first(place(0), kvs, qs, w_out)
    acc_b, peak_b = own_second(k_all, v_all, q_all)
    own = (acc_a, peak_a, acc_b, peak_b)
    attended = past_part(place(0), beta, past, q_all, own, (window, after))
    heads = [attended[0]] + [None] * (NB - 1)
    for d in LEAVE:
        heads[d] = shifted(attended[d], PLANE, NB - d)

    def send(part, distance):
        return shifted(part, "head", distance)

    far_up, far_low = project(place(2), heads, weight, BF16, BF16)
    far_up, far_low = send(far_up, 1), send(far_low, -1)
    right_up, right_low = project(place(1), heads, weight, F32, BF16)
    got_low = send(right_low, 1)
    left_up, left_low = project(place(3), heads, weight, BF16, F32)
    got_up = send(left_up, -1)
    more_up = send(added(right_up, far_up, BF16), 1)
    more_low = send(added(left_low, far_low, BF16), -1)
    own_up, own_low = project(place(0), heads, weight, F32, F32)
    return finish(own_up, own_low, got_up, more_up, got_low, more_low)


def solution(mesh):
    torus = Mesh(
        mesh.devices.reshape(8, 4, 2, mesh.shape["head"]), ("seq_0", "seq_1", "seq_2", "head")
    )
    seq = ("seq_0", "seq_1", "seq_2")
    return jax.shard_map(
        layer,
        mesh=torus,
        in_specs=(P(seq, "head"), P(seq, "head"), P(seq, "head"), P("head"), P("head", None)),
        out_specs=P(seq, "head"),
        check_vma=False,
    )
```

```python
import jax
import jax.numpy as jnp
from jax import lax
from jax.experimental import pallas as pl
from jax.experimental.pallas import tpu as pltpu
from jax.sharding import Mesh
from jax.sharding import PartitionSpec as P


HD = 128
BLK = 256
NB = 8
PLANE = ("seq_1", "seq_2")
SCALE2 = (HD**-0.5) * 1.4426950408889634
F32 = jnp.float32
BF16 = jnp.bfloat16
ANY = pl.BlockSpec(memory_space=pl.ANY)
SMEM = pl.BlockSpec(memory_space=pltpu.SMEM)
VMEM = pl.BlockSpec(memory_space=pltpu.VMEM)
HBM = pl.BlockSpec(memory_space=pltpu.HBM)
NY = 4
PAIR = 2 * BLK
STEPS = (1, 3, 2)
LEAVE = (2, 1, 3)
SPLIT = 6


def shifted(block, axis, distance, wrap=True):
    size = lax.axis_size(axis)
    if wrap:
        route = [(i, (i + distance) % size) for i in range(size)]
    else:
        route = [(i, i + distance) for i in range(size - distance)]
    return lax.ppermute(block, axis, route)


def elu_plus(inputs):
    return jnp.where(inputs > 0, inputs + 1.0, jnp.exp(jnp.minimum(inputs, 0.0)))


def pair_rows(here, step, half):
    row = lax.rem(here // 2 - step + NY, NY) * PAIR + half * BLK
    return pl.ds(pl.multiple_of(row, BLK), BLK)


def params(flops, nbytes, room=16):
    return dict(
        cost_estimate=pl.CostEstimate(flops=flops, bytes_accessed=nbytes, transcendentals=0),
        compiler_params=pltpu.CompilerParams(vmem_limit_bytes=room * 1024 * 1024),
    )


def split_kernel(here_ref, keys, values, queries, stay, leave, whole, sems):
    here = here_ref[0]
    copies = [
        pltpu.make_async_copy(array, whole.at[n], sems.at[n])
        for n, array in enumerate((keys, values, queries))
    ]
    for copy in copies:
        copy.start()
    own_core = lax.rem(here, 2)
    for n, copy in enumerate(copies):
        copy.wait()
        for step in range(NY):
            pair = lax.rem(here // 2 + step, NY) * 2
            for out, core in ((leave, 1 - own_core), (stay, own_core)):
                cols = pl.ds(pl.multiple_of((pair + core) * HD, HD), HD)
                out[step, n] = whole[n, :, cols]


def split_heads(here, keys, values, queries):
    half = jax.ShapeDtypeStruct((NY, 3, BLK, HD), BF16)
    return pl.pallas_call(
        split_kernel,
        out_shape=(half, half),
        in_specs=[SMEM] + [HBM] * 3,
        out_specs=(VMEM, VMEM),
        scratch_shapes=[
            pltpu.VMEM((3, BLK, NB * HD), BF16),
            pltpu.SemaphoreType.DMA((3,)),
        ],
        name="split",
        **params(0, 3 << 20),
    )(here, keys, values, queries)


def pair_kernel(*refs):
    here_ref, stay, got = refs[:3]
    kvs, qs = refs[3 : 3 + NY], refs[3 + NY : 3 + 2 * NY]
    core = lax.rem(here_ref[0], 2)
    for step in range(NY):
        for part, half in ((stay, core), (got, 1 - core)):
            kvs[step][half] = part[step, 0:2]
            qs[step][half] = part[step, 2]


def pair_up(here, stay, got):
    out = pl.pallas_call(
        pair_kernel,
        out_shape=[jax.ShapeDtypeStruct((2, 2, BLK, HD), BF16)] * NY
        + [jax.ShapeDtypeStruct((2, BLK, HD), BF16)] * NY,
        in_specs=[SMEM, VMEM, VMEM],
        out_specs=[VMEM] * (2 * NY),
        name="pair_up",
        **params(0, 3 << 20),
    )(here, stay, got)
    return out[:NY], out[NY:]


def pack_kernel(first, second, out):
    out[0] = first[...]
    out[1] = second[...]


def pack(first, second):
    return pl.pallas_call(
        pack_kernel,
        out_shape=jax.ShapeDtypeStruct((2, *first.shape), BF16),
        in_specs=[VMEM, VMEM],
        out_specs=VMEM,
        name="pack",
        **params(0, 1 << 20),
    )(first, second)


def terms_kernel(*refs):
    pieces, out, wire = refs[:NY], refs[NY], refs[NY + 1]
    outer = jnp.zeros((HD, HD), F32)
    totals = jnp.zeros((8, HD), F32)
    for piece in pieces:
        for half in range(2):
            soft = elu_plus(piece[half, 0].astype(F32)).astype(BF16)
            outer = outer + lax.dot_general(
                soft, piece[half, 1], (((0,), (0,)), ((), ())), preferred_element_type=F32
            )
            totals = totals + jnp.dot(jnp.ones((8, BLK), BF16), soft, preferred_element_type=F32)
    out[0:HD, :] = outer
    out[HD : HD + 8, :] = totals
    wire[0:HD, :] = outer.astype(BF16)
    wire[HD : HD + 8, :] = totals.astype(BF16)


def memory_terms(pieces):
    return pl.pallas_call(
        terms_kernel,
        out_shape=(
            jax.ShapeDtypeStruct((HD + 8, HD), F32),
            jax.ShapeDtypeStruct((HD + 8, HD), BF16),
        ),
        in_specs=[VMEM] * NY,
        out_specs=(VMEM, VMEM),
        name="terms",
        **params(2 * 2048 * HD * HD, 1 << 20),
    )(*pieces)


def attend(query, keys, values_ones, scores, first, count, mask_at, mask, start_max=None):
    peak = start_max
    for j in range(count):
        rows = pl.ds((first + j) * BLK, BLK)
        part = lax.dot_general(
            query, keys[rows, :], (((1,), (1,)), ((), ())), preferred_element_type=F32
        )
        if j == mask_at:
            part = jnp.where(mask, part, -jnp.inf)
        scores[:, j * BLK : (j + 1) * BLK] = part
        high = jnp.maximum(part[:, :HD], part[:, HD:])
        peak = high if peak is None else jnp.maximum(peak, high)
    peak = jnp.max(peak, axis=1, keepdims=True)
    half = query.shape[0] // 2
    upper = lower = None
    for j in range(count):
        rows = pl.ds((first + j) * BLK, BLK)
        weights = scores[:, j * BLK : (j + 1) * BLK] - peak
        weights = jnp.exp2(weights * SCALE2).astype(BF16)
        value = values_ones[rows, :]
        above = jnp.dot(weights[:half], value, preferred_element_type=F32)
        below = jnp.dot(weights[half:], value, preferred_element_type=F32)
        upper = above if upper is None else upper + above
        lower = below if lower is None else lower + below
    acc = jnp.concatenate([upper, lower], axis=0)
    return acc, peak


def tile_mask():
    row = lax.broadcasted_iota(jnp.int32, (BLK, BLK), 0)
    col = lax.broadcasted_iota(jnp.int32, (BLK, BLK), 1)
    return col <= row


def own_blocks(blocks, query, keys, values, scores, acc_out, peak_out):
    mask = tile_mask()
    for n, b in enumerate(blocks):
        acc, peak = attend(
            query[pl.ds(b * BLK, BLK), :], keys, values, scores[n % 2], 0, b + 1, b, mask
        )
        rows = pl.ds(n * BLK, BLK)
        acc_out[rows, :] = acc
        peak_out[rows, :] = jnp.broadcast_to(peak, (BLK, HD))


def own_first_kernel(*refs):
    here_ref, kvs, qs = refs[0], refs[1 : 1 + NY], refs[1 + NY : 1 + 2 * NY]
    weight, keys, values, query, acc_out, peak_out, weight_out = refs[1 + 2 * NY : 8 + 2 * NY]
    scores_a, scores_b, sem = refs[8 + 2 * NY :]
    fetch = pltpu.make_async_copy(weight, weight_out, sem)
    fetch.start()
    here = here_ref[0]
    for step in range(NY):
        for half in range(2):
            rows = pair_rows(here, step, half)
            keys[rows, :] = kvs[step][half, 0]
            values[rows, :HD] = kvs[step][half, 1]
            query[rows, :] = qs[step][half]
    values[:, HD:] = jnp.ones((NB * BLK, HD), BF16)
    own_blocks(range(SPLIT), query, keys, values, (scores_a, scores_b), acc_out, peak_out)
    fetch.wait()


def own_second_kernel(keys, values, query, acc_out, peak_out, scores_a, scores_b):
    own_blocks(range(SPLIT, NB), query, keys, values, (scores_a, scores_b), acc_out, peak_out)


def own_first(here, kvs, qs, weight):
    rows = NB * BLK
    return pl.pallas_call(
        own_first_kernel,
        out_shape=(
            jax.ShapeDtypeStruct((rows, HD), BF16),
            jax.ShapeDtypeStruct((rows, 2 * HD), BF16),
            jax.ShapeDtypeStruct((rows, HD), BF16),
            jax.ShapeDtypeStruct((SPLIT * BLK, 2 * HD), F32),
            jax.ShapeDtypeStruct((SPLIT * BLK, HD), F32),
            jax.ShapeDtypeStruct(weight.shape, BF16),
        ),
        in_specs=[SMEM] + [VMEM] * (2 * NY) + [HBM],
        out_specs=(VMEM,) * 6,
        scratch_shapes=[
            pltpu.VMEM((BLK, SPLIT * BLK), F32),
            pltpu.VMEM((BLK, SPLIT * BLK), F32),
            pltpu.SemaphoreType.DMA,
        ],
        name="own_first",
        **params(21 * BLK * BLK * HD * 8, 5 << 20),
    )(here, *kvs, *qs, weight)


def own_second(keys, values, query):
    rows = NB * BLK
    return pl.pallas_call(
        own_second_kernel,
        out_shape=(
            jax.ShapeDtypeStruct((rows - SPLIT * BLK, 2 * HD), F32),
            jax.ShapeDtypeStruct((rows - SPLIT * BLK, HD), F32),
        ),
        in_specs=[VMEM] * 3,
        out_specs=(VMEM, VMEM),
        scratch_shapes=[pltpu.VMEM((BLK, rows), F32)] * 2,
        name="own_second",
        **params(15 * BLK * BLK * HD * 8, 3 << 20),
    )(keys, values, query)


def prefix_kernel(place_ref, terms, after, chosen, kept):
    segment = place_ref[1]
    passed = after[...].astype(F32)
    whole = terms[...] + passed
    wrapped = jnp.where(segment == 7, passed, 0.0)
    chosen[...] = jnp.where(segment <= 5, whole, wrapped).astype(BF16)
    kept[...] = jnp.where(segment <= 3, whole, wrapped)


def prefix_step(place, terms, after):
    shape = jax.ShapeDtypeStruct(terms.shape, F32)
    return pl.pallas_call(
        prefix_kernel,
        out_shape=(jax.ShapeDtypeStruct(terms.shape, BF16), shape),
        in_specs=[SMEM, VMEM, VMEM],
        out_specs=(VMEM, VMEM),
        name="prefix",
        **params(0, 1 << 18),
    )(place, terms, after)


def window_kernel(kept, after, out, wire):
    out[...] = kept[...] + after[...].astype(F32)
    wire[...] = out[...].astype(BF16)


def window_step(kept, after):
    return pl.pallas_call(
        window_kernel,
        out_shape=(
            jax.ShapeDtypeStruct(kept.shape, F32),
            jax.ShapeDtypeStruct(kept.shape, BF16),
        ),
        in_specs=[VMEM, VMEM],
        out_specs=(VMEM, VMEM),
        name="window",
        **params(0, 1 << 18),
    )(kept, after)


def add_kernel(left, right, out):
    out[...] = (left[...] + right[...].astype(F32)).astype(out.dtype)


def added(left, right, dtype):
    return pl.pallas_call(
        add_kernel,
        out_shape=jax.ShapeDtypeStruct(left.shape, dtype),
        in_specs=[VMEM, VMEM],
        out_specs=VMEM,
        name="added",
        **params(0, 1 << 18),
    )(left, right)


def past_kernel(*refs):
    here_ref, same, near, far, query = refs[:5]
    acc_a, peak_a, acc_b, peak_b, local_out = refs[5:10]
    keys, values, scores_a, scores_b, acc_buf = refs[10:]
    here, segment = here_ref[0], here_ref[1]

    def own(b):
        if b < SPLIT:
            rows = pl.ds(b * BLK, BLK)
            return acc_a, peak_a, rows
        return acc_b, peak_b, pl.ds((b - SPLIT) * BLK, BLK)

    @pl.when(segment == 0)
    def _():
        acc_buf[: SPLIT * BLK, :] = acc_a[...]
        acc_buf[SPLIT * BLK :, :] = acc_b[...]

    @pl.when(segment > 0)
    def _():
        for step, part in ((0, same), (1, near.at[0]), (3, near.at[1]), (2, far)):
            for half in range(2):
                rows = pair_rows(here, step, half)
                keys[rows, :] = part[half, 0]
                values[rows, :HD] = part[half, 1]
        values[:, HD:] = jnp.ones((NB * BLK, HD), BF16)
        mask = jnp.logical_not(tile_mask())
        for b in range(NB):
            rows = pl.ds(b * BLK, BLK)
            acc_in, peak_in, own_rows = own(b)
            before = peak_in[own_rows, :]
            acc, peak = attend(
                query[rows, :],
                keys,
                values,
                (scores_a, scores_b)[b % 2],
                b,
                NB - b,
                0,
                mask,
                before,
            )
            fade = jnp.exp2((before - peak) * SCALE2)
            acc_buf[rows, :HD] = acc[:, :HD] + acc_in[own_rows, :HD] * fade
            acc_buf[rows, HD:] = acc[:, HD:] + acc_in[own_rows, HD:] * fade

    local_out[...] = acc_buf[:, :HD] / acc_buf[:, HD:]


def blend_kernel(*refs):
    here_ref, beta_ref, query, local_ref, memory_ref, more_ref = refs[:6]
    outs, result = refs[6:-1], refs[-1]
    here, segment = here_ref[0], here_ref[1]
    total = jnp.where(segment <= 3, 0.0, memory_ref[...]) + more_ref[...].astype(F32)
    memory = total[0:HD, :]
    norm = jnp.transpose(jnp.broadcast_to(total[HD : HD + 1, :], (HD, HD)))
    whole = jnp.concatenate([memory, norm], axis=1)
    upper = whole.astype(BF16)
    lower = (whole - upper.astype(F32)).astype(BF16)
    split = jnp.concatenate([upper, lower], axis=0)
    gate = 1.0 / (1.0 + jnp.exp(-jnp.full((1, HD), beta_ref[here], F32)))
    for b in range(NB):
        rows = pl.ds(b * BLK, BLK)
        soft = elu_plus(query[rows, :].astype(F32)).astype(BF16)
        both = jnp.dot(jnp.concatenate([soft, soft], axis=1), split, preferred_element_type=F32)
        from_memory = both[:, :HD] / (1.0 + both[:, HD:])
        local = local_ref[rows, :]
        result[rows, :] = (gate * from_memory + (1.0 - gate) * local).astype(BF16)
    for step in range(NY):
        for half in range(2):
            outs[step][half] = result[pair_rows(here, step, half), :]


def past_part(here, past, query, own):
    rows = NB * BLK
    return pl.pallas_call(
        past_kernel,
        out_shape=jax.ShapeDtypeStruct((rows, HD), F32),
        in_specs=[SMEM] + [VMEM] * 8,
        out_specs=VMEM,
        scratch_shapes=[
            pltpu.VMEM((rows, HD), BF16),
            pltpu.VMEM((rows, 2 * HD), BF16),
            pltpu.VMEM((BLK, rows), F32),
            pltpu.VMEM((BLK, rows), F32),
            pltpu.VMEM((rows, 2 * HD), F32),
        ],
        name="past",
        **params(36 * BLK * BLK * HD * 8, 6 << 20, 24),
    )(here, *past, query, *own)


def blend(here, beta, query, local, memory):
    return pl.pallas_call(
        blend_kernel,
        out_shape=[jax.ShapeDtypeStruct((2, BLK, HD), BF16)] * NY,
        in_specs=[SMEM, SMEM] + [VMEM] * 4,
        out_specs=[VMEM] * NY,
        scratch_shapes=[pltpu.VMEM((NB * BLK, HD), BF16)],
        name="blend",
        **params(1 << 28, 3 << 20),
    )(here, beta, query, local, *memory)


def turn_kernel(*refs):
    core = lax.rem(refs[0][0], 2)
    for step in range(NY):
        refs[-1][step] = refs[1 + step][1 - core]


def turn(here, pieces):
    return pl.pallas_call(
        turn_kernel,
        out_shape=jax.ShapeDtypeStruct((NY, BLK, HD), BF16),
        in_specs=[SMEM] + [VMEM] * NY,
        out_specs=VMEM,
        name="turn",
        **params(0, 1 << 18),
    )(here, *pieces)


def project_kernel(*refs):
    spot_ref = refs[0]
    pieces, other, weight = refs[1 : 1 + NY], refs[1 + NY], refs[2 + NY]
    upper, lower = refs[3 + NY : 5 + NY]
    attended = refs[5 + NY]
    core = lax.rem(spot_ref[0], 2)
    for step in range(NY):
        pair = lax.rem(spot_ref[0] // 2 + step, NY) * 2
        start = pl.multiple_of((pair + core) * HD, HD)
        attended[:, pl.ds(start, HD)] = pieces[step][core]
        start = pl.multiple_of((pair + 1 - core) * HD, HD)
        attended[:, pl.ds(start, HD)] = other[step]
    width = upper.shape[1]
    cols = pl.ds(pl.multiple_of(lax.rem(spot_ref[2] + spot_ref[3], 4) * width, width), width)
    whole = jnp.dot(attended[...], weight[:, cols], preferred_element_type=F32)
    upper[...] = whole[: BLK // 2].astype(upper.dtype)
    lower[...] = whole[BLK // 2 :].astype(lower.dtype)


def project(place, pieces, weight, upper, lower):
    width = weight.shape[1] // 4
    return pl.pallas_call(
        project_kernel,
        in_specs=[SMEM] + [VMEM] * (2 + NY),
        out_specs=(VMEM, VMEM),
        scratch_shapes=[pltpu.VMEM((BLK, NB * HD), BF16)],
        out_shape=(
            jax.ShapeDtypeStruct((BLK // 2, width), upper),
            jax.ShapeDtypeStruct((BLK // 2, width), lower),
        ),
        name="project",
        **params(2 * BLK * NB * HD * width, 3 << 20),
    )(place, *pieces, weight)


def finish_kernel(own_up, own_low, up_a, up_b, low_a, low_b, out):
    half = BLK // 2
    out[:half] = (own_up[...] + up_a[...].astype(F32) + up_b[...].astype(F32)).astype(BF16)
    out[half:] = (own_low[...] + low_a[...].astype(F32) + low_b[...].astype(F32)).astype(BF16)


def finish(*parts):
    return pl.pallas_call(
        finish_kernel,
        in_specs=[VMEM] * 6,
        out_specs=VMEM,
        out_shape=jax.ShapeDtypeStruct((BLK, parts[0].shape[1]), BF16),
        name="finish",
        **params(0, 3 << 20),
    )(*parts)


def layer(queries, keys, values, beta, w_out):
    here = lax.axis_index(PLANE)
    segment = lax.axis_index("seq_0")
    column = lax.axis_index("head")

    def place(e):
        return jnp.stack((here, segment, column, e)).astype(jnp.int32)

    keys, values, queries, w_out = (
        pltpu.with_memory_space_constraint(part, pltpu.HBM)
        for part in (keys, values, queries, w_out)
    )
    stay, leave = split_heads(place(0), keys, values, queries)
    got = shifted(leave, "seq_2", 1)
    kvs, qs = map(list, pair_up(place(0), stay, got))
    past = [shifted(kvs[0], "seq_0", 1)]
    for step in STEPS:
        kvs[step] = shifted(kvs[step], "seq_1", step)
    past.append(shifted(pack(kvs[1], kvs[3]), "seq_0", 1))
    past.append(shifted(kvs[2], "seq_0", 1))
    for step in STEPS:
        qs[step] = shifted(qs[step], "seq_1", step)

    terms, wire = memory_terms(kvs)
    after = shifted(wire, "seq_0", -1)
    chosen, kept = prefix_step(place(0), terms, after)
    after = shifted(chosen, "seq_0", -2)
    window, wire = window_step(kept, after)
    after = shifted(wire, "seq_0", -4)

    k_all, v_all, q_all, acc_a, peak_a, weight = own_first(place(0), kvs, qs, w_out)
    acc_b, peak_b = own_second(k_all, v_all, q_all)
    own = (acc_a, peak_a, acc_b, peak_b)
    local = past_part(place(0), past, q_all, own)
    attended = blend(place(0), beta, q_all, local, (window, after))
    heads = list(attended)
    for step in LEAVE:
        heads[step] = shifted(heads[step], "seq_1", -step)
    heads.append(shifted(turn(place(0), heads), "seq_2", 1))

    def send(part, distance):
        return shifted(part, "head", distance)

    far_up, far_low = project(place(2), heads, weight, BF16, BF16)
    far_up, far_low = send(far_up, 1), send(far_low, -1)
    right_up, right_low = project(place(1), heads, weight, F32, BF16)
    got_low = send(right_low, 1)
    left_up, left_low = project(place(3), heads, weight, BF16, F32)
    got_up = send(left_up, -1)
    more_up = send(added(right_up, far_up, BF16), 1)
    more_low = send(added(left_low, far_low, BF16), -1)
    own_up, own_low = project(place(0), heads, weight, F32, F32)
    return finish(own_up, own_low, got_up, more_up, got_low, more_low)


def solution(mesh):
    torus = Mesh(
        mesh.devices.reshape(8, 4, 2, mesh.shape["head"]), ("seq_0", "seq_1", "seq_2", "head")
    )
    seq = ("seq_0", "seq_1", "seq_2")
    return jax.shard_map(
        layer,
        mesh=torus,
        in_specs=(P(seq, "head"), P(seq, "head"), P(seq, "head"), P("head"), P("head", None)),
        out_specs=P(seq, "head"),
        check_vma=False,
    )
```

```python
import jax
import jax.numpy as jnp
from jax import lax
from jax.experimental import pallas as pl
from jax.experimental.pallas import tpu as pltpu
from jax.sharding import Mesh
from jax.sharding import PartitionSpec as P


HD = 128
BLK = 256
NB = 8
PLANE = ("seq_1", "seq_2")
SCALE2 = (HD**-0.5) * 1.4426950408889634
F32 = jnp.float32
BF16 = jnp.bfloat16
ANY = pl.BlockSpec(memory_space=pl.ANY)
SMEM = pl.BlockSpec(memory_space=pltpu.SMEM)
VMEM = pl.BlockSpec(memory_space=pltpu.VMEM)
HBM = pl.BlockSpec(memory_space=pltpu.HBM)
NY = 4
PAIR = 2 * BLK
STEPS = (1, 3, 2)
LEAVE = (2, 1, 3)
SPLIT = 6


def shifted(block, axis, distance, wrap=True):
    size = lax.axis_size(axis)
    if wrap:
        route = [(i, (i + distance) % size) for i in range(size)]
    else:
        route = [(i, i + distance) for i in range(size - distance)]
    return lax.ppermute(block, axis, route)


def elu_plus(inputs):
    return jnp.where(inputs > 0, inputs + 1.0, jnp.exp(jnp.minimum(inputs, 0.0)))


def pair_rows(here, step, half):
    row = lax.rem(here // 2 - step + NY, NY) * PAIR + half * BLK
    return pl.ds(pl.multiple_of(row, BLK), BLK)


def params(flops, nbytes, room=16):
    return dict(
        cost_estimate=pl.CostEstimate(flops=flops, bytes_accessed=nbytes, transcendentals=0),
        compiler_params=pltpu.CompilerParams(vmem_limit_bytes=room * 1024 * 1024),
    )


def split_kernel(here_ref, keys, values, queries, stay, leave, whole, sems):
    here = here_ref[0]
    copies = [
        pltpu.make_async_copy(array, whole.at[n], sems.at[n])
        for n, array in enumerate((keys, values, queries))
    ]
    for copy in copies:
        copy.start()
    own_core = lax.rem(here, 2)
    for n, copy in enumerate(copies):
        copy.wait()
        for step in range(NY):
            pair = lax.rem(here // 2 + step, NY) * 2
            for out, core in ((leave, 1 - own_core), (stay, own_core)):
                cols = pl.ds(pl.multiple_of((pair + core) * HD, HD), HD)
                out[step, n] = whole[n, :, cols]


def split_heads(here, keys, values, queries):
    half = jax.ShapeDtypeStruct((NY, 3, BLK, HD), BF16)
    return pl.pallas_call(
        split_kernel,
        out_shape=(half, half),
        in_specs=[SMEM] + [HBM] * 3,
        out_specs=(VMEM, VMEM),
        scratch_shapes=[
            pltpu.VMEM((3, BLK, NB * HD), BF16),
            pltpu.SemaphoreType.DMA((3,)),
        ],
        name="split",
        **params(0, 3 << 20),
    )(here, keys, values, queries)


def pair_kernel(*refs):
    here_ref, stay, got = refs[:3]
    kvs, qs = refs[3 : 3 + NY], refs[3 + NY : 3 + 2 * NY]
    core = lax.rem(here_ref[0], 2)
    for step in range(NY):
        for part, half in ((stay, core), (got, 1 - core)):
            kvs[step][half] = part[step, 0:2]
            qs[step][half] = part[step, 2]


def pair_up(here, stay, got):
    out = pl.pallas_call(
        pair_kernel,
        out_shape=[jax.ShapeDtypeStruct((2, 2, BLK, HD), BF16)] * NY
        + [jax.ShapeDtypeStruct((2, BLK, HD), BF16)] * NY,
        in_specs=[SMEM, VMEM, VMEM],
        out_specs=[VMEM] * (2 * NY),
        name="pair_up",
        **params(0, 3 << 20),
    )(here, stay, got)
    return out[:NY], out[NY:]


def pack_kernel(first, second, out):
    out[0] = first[...]
    out[1] = second[...]


def pack(first, second):
    return pl.pallas_call(
        pack_kernel,
        out_shape=jax.ShapeDtypeStruct((2, *first.shape), BF16),
        in_specs=[VMEM, VMEM],
        out_specs=VMEM,
        name="pack",
        **params(0, 1 << 20),
    )(first, second)


def terms_kernel(*refs):
    pieces, out, wire = refs[:NY], refs[NY], refs[NY + 1]
    outer = jnp.zeros((HD, HD), F32)
    totals = jnp.zeros((8, HD), F32)
    for piece in pieces:
        for half in range(2):
            soft = elu_plus(piece[half, 0].astype(F32)).astype(BF16)
            outer = outer + lax.dot_general(
                soft, piece[half, 1], (((0,), (0,)), ((), ())), preferred_element_type=F32
            )
            totals = totals + jnp.dot(jnp.ones((8, BLK), BF16), soft, preferred_element_type=F32)
    out[0:HD, :] = outer
    out[HD : HD + 8, :] = totals
    wire[0:HD, :] = outer.astype(BF16)
    wire[HD : HD + 8, :] = totals.astype(BF16)


def memory_terms(pieces):
    return pl.pallas_call(
        terms_kernel,
        out_shape=(
            jax.ShapeDtypeStruct((HD + 8, HD), F32),
            jax.ShapeDtypeStruct((HD + 8, HD), BF16),
        ),
        in_specs=[VMEM] * NY,
        out_specs=(VMEM, VMEM),
        name="terms",
        **params(2 * 2048 * HD * HD, 1 << 20),
    )(*pieces)


def attend(query, keys, values_ones, scores, first, count, mask_at, mask, start_max=None):
    peak = start_max
    for j in range(count):
        rows = pl.ds((first + j) * BLK, BLK)
        part = lax.dot_general(
            query, keys[rows, :], (((1,), (1,)), ((), ())), preferred_element_type=F32
        )
        if j == mask_at:
            part = jnp.where(mask, part, -jnp.inf)
        scores[:, j * BLK : (j + 1) * BLK] = part
        high = jnp.maximum(part[:, :HD], part[:, HD:])
        peak = high if peak is None else jnp.maximum(peak, high)
    peak = jnp.max(peak, axis=1, keepdims=True)
    half = query.shape[0] // 2
    upper = lower = None
    for j in range(count):
        rows = pl.ds((first + j) * BLK, BLK)
        weights = scores[:, j * BLK : (j + 1) * BLK] - peak
        weights = jnp.exp2(weights * SCALE2).astype(BF16)
        value = values_ones[rows, :]
        above = jnp.dot(weights[:half], value, preferred_element_type=F32)
        below = jnp.dot(weights[half:], value, preferred_element_type=F32)
        upper = above if upper is None else upper + above
        lower = below if lower is None else lower + below
    acc = jnp.concatenate([upper, lower], axis=0)
    return acc, peak


def tile_mask():
    row = lax.broadcasted_iota(jnp.int32, (BLK, BLK), 0)
    col = lax.broadcasted_iota(jnp.int32, (BLK, BLK), 1)
    return col <= row


def own_blocks(blocks, query, keys, values, scores, acc_out, peak_out):
    mask = tile_mask()
    for n, b in enumerate(blocks):
        acc, peak = attend(
            query[pl.ds(b * BLK, BLK), :], keys, values, scores[n % 2], 0, b + 1, b, mask
        )
        rows = pl.ds(n * BLK, BLK)
        acc_out[rows, :] = acc
        peak_out[rows, :] = jnp.broadcast_to(peak, (BLK, HD))


def own_first_kernel(*refs):
    here_ref, kvs, qs = refs[0], refs[1 : 1 + NY], refs[1 + NY : 1 + 2 * NY]
    keys, values, query, acc_out, peak_out = refs[1 + 2 * NY : 6 + 2 * NY]
    scores_a, scores_b = refs[6 + 2 * NY :]
    here = here_ref[0]
    for step in range(NY):
        for half in range(2):
            rows = pair_rows(here, step, half)
            keys[rows, :] = kvs[step][half, 0]
            values[rows, :HD] = kvs[step][half, 1]
            query[rows, :] = qs[step][half]
    values[:, HD:] = jnp.ones((NB * BLK, HD), BF16)
    own_blocks(range(SPLIT), query, keys, values, (scores_a, scores_b), acc_out, peak_out)


def own_second_kernel(keys, values, query, acc_out, peak_out, scores_a, scores_b):
    own_blocks(range(SPLIT, NB), query, keys, values, (scores_a, scores_b), acc_out, peak_out)


def own_first(here, kvs, qs):
    rows = NB * BLK
    return pl.pallas_call(
        own_first_kernel,
        out_shape=(
            jax.ShapeDtypeStruct((rows, HD), BF16),
            jax.ShapeDtypeStruct((rows, 2 * HD), BF16),
            jax.ShapeDtypeStruct((rows, HD), BF16),
            jax.ShapeDtypeStruct((SPLIT * BLK, 2 * HD), F32),
            jax.ShapeDtypeStruct((SPLIT * BLK, HD), F32),
        ),
        in_specs=[SMEM] + [VMEM] * (2 * NY),
        out_specs=(VMEM,) * 5,
        scratch_shapes=[
            pltpu.VMEM((BLK, SPLIT * BLK), F32),
            pltpu.VMEM((BLK, SPLIT * BLK), F32),
        ],
        name="own_first",
        **params(21 * BLK * BLK * HD * 8, 5 << 20),
    )(here, *kvs, *qs)


def own_second(keys, values, query):
    rows = NB * BLK
    return pl.pallas_call(
        own_second_kernel,
        out_shape=(
            jax.ShapeDtypeStruct((rows - SPLIT * BLK, 2 * HD), F32),
            jax.ShapeDtypeStruct((rows - SPLIT * BLK, HD), F32),
        ),
        in_specs=[VMEM] * 3,
        out_specs=(VMEM, VMEM),
        scratch_shapes=[pltpu.VMEM((BLK, rows), F32)] * 2,
        name="own_second",
        **params(15 * BLK * BLK * HD * 8, 3 << 20),
    )(keys, values, query)


def prefix_kernel(place_ref, terms, after, chosen, kept):
    segment = place_ref[1]
    passed = after[...].astype(F32)
    whole = terms[...] + passed
    wrapped = jnp.where(segment == 7, passed, 0.0)
    chosen[...] = jnp.where(segment <= 5, whole, wrapped).astype(BF16)
    kept[...] = jnp.where(segment <= 3, whole, wrapped)


def prefix_step(place, terms, after):
    shape = jax.ShapeDtypeStruct(terms.shape, F32)
    return pl.pallas_call(
        prefix_kernel,
        out_shape=(jax.ShapeDtypeStruct(terms.shape, BF16), shape),
        in_specs=[SMEM, VMEM, VMEM],
        out_specs=(VMEM, VMEM),
        name="prefix",
        **params(0, 1 << 18),
    )(place, terms, after)


def window_kernel(kept, after, out, wire):
    out[...] = kept[...] + after[...].astype(F32)
    wire[...] = out[...].astype(BF16)


def window_step(kept, after):
    return pl.pallas_call(
        window_kernel,
        out_shape=(
            jax.ShapeDtypeStruct(kept.shape, F32),
            jax.ShapeDtypeStruct(kept.shape, BF16),
        ),
        in_specs=[VMEM, VMEM],
        out_specs=(VMEM, VMEM),
        name="window",
        **params(0, 1 << 18),
    )(kept, after)


def add_kernel(left, right, out):
    out[...] = (left[...] + right[...].astype(F32)).astype(out.dtype)


def added(left, right, dtype):
    return pl.pallas_call(
        add_kernel,
        out_shape=jax.ShapeDtypeStruct(left.shape, dtype),
        in_specs=[VMEM, VMEM],
        out_specs=VMEM,
        name="added",
        **params(0, 1 << 18),
    )(left, right)


def past_kernel(*refs):
    here_ref, same, near, far, query = refs[:5]
    acc_a, peak_a, acc_b, peak_b, weight, local_out, weight_out = refs[5:12]
    keys, values, scores_a, scores_b, acc_buf, sem = refs[12:]
    fetch = pltpu.make_async_copy(weight, weight_out, sem)
    fetch.start()
    here, segment = here_ref[0], here_ref[1]

    def own(b):
        if b < SPLIT:
            rows = pl.ds(b * BLK, BLK)
            return acc_a, peak_a, rows
        return acc_b, peak_b, pl.ds((b - SPLIT) * BLK, BLK)

    @pl.when(segment == 0)
    def _():
        acc_buf[: SPLIT * BLK, :] = acc_a[...]
        acc_buf[SPLIT * BLK :, :] = acc_b[...]

    @pl.when(segment > 0)
    def _():
        for step, part in ((0, same), (1, near.at[0]), (3, near.at[1]), (2, far)):
            for half in range(2):
                rows = pair_rows(here, step, half)
                keys[rows, :] = part[half, 0]
                values[rows, :HD] = part[half, 1]
        values[:, HD:] = jnp.ones((NB * BLK, HD), BF16)
        mask = jnp.logical_not(tile_mask())
        for b in range(NB):
            rows = pl.ds(b * BLK, BLK)
            acc_in, peak_in, own_rows = own(b)
            before = peak_in[own_rows, :]
            acc, peak = attend(
                query[rows, :],
                keys,
                values,
                (scores_a, scores_b)[b % 2],
                b,
                NB - b,
                0,
                mask,
                before,
            )
            fade = jnp.exp2((before - peak) * SCALE2)
            acc_buf[rows, :HD] = acc[:, :HD] + acc_in[own_rows, :HD] * fade
            acc_buf[rows, HD:] = acc[:, HD:] + acc_in[own_rows, HD:] * fade

    local_out[...] = acc_buf[:, :HD] / acc_buf[:, HD:]
    fetch.wait()


def blend_kernel(*refs):
    here_ref, beta_ref, query, local_ref, memory_ref, more_ref = refs[:6]
    outs, result = refs[6:-1], refs[-1]
    here, segment = here_ref[0], here_ref[1]
    total = jnp.where(segment <= 3, 0.0, memory_ref[...]) + more_ref[...].astype(F32)
    memory = total[0:HD, :]
    norm = jnp.transpose(jnp.broadcast_to(total[HD : HD + 1, :], (HD, HD)))
    whole = jnp.concatenate([memory, norm], axis=1)
    upper = whole.astype(BF16)
    lower = (whole - upper.astype(F32)).astype(BF16)
    split = jnp.concatenate([upper, lower], axis=0)
    gate = 1.0 / (1.0 + jnp.exp(-jnp.full((1, HD), beta_ref[here], F32)))
    for b in range(NB):
        rows = pl.ds(b * BLK, BLK)
        soft = elu_plus(query[rows, :].astype(F32)).astype(BF16)
        both = jnp.dot(jnp.concatenate([soft, soft], axis=1), split, preferred_element_type=F32)
        from_memory = both[:, :HD] / (1.0 + both[:, HD:])
        local = local_ref[rows, :]
        result[rows, :] = (gate * from_memory + (1.0 - gate) * local).astype(BF16)
    for step in range(NY):
        for half in range(2):
            outs[step][half] = result[pair_rows(here, step, half), :]


def past_part(here, past, query, own, weight):
    rows = NB * BLK
    return pl.pallas_call(
        past_kernel,
        out_shape=(
            jax.ShapeDtypeStruct((rows, HD), F32),
            jax.ShapeDtypeStruct(weight.shape, BF16),
        ),
        in_specs=[SMEM] + [VMEM] * 8 + [HBM],
        out_specs=(VMEM, VMEM),
        scratch_shapes=[
            pltpu.VMEM((rows, HD), BF16),
            pltpu.VMEM((rows, 2 * HD), BF16),
            pltpu.VMEM((BLK, rows), F32),
            pltpu.VMEM((BLK, rows), F32),
            pltpu.VMEM((rows, 2 * HD), F32),
            pltpu.SemaphoreType.DMA,
        ],
        name="past",
        **params(36 * BLK * BLK * HD * 8, 6 << 20, 24),
    )(here, *past, query, *own, weight)


def blend(here, beta, query, local, memory):
    return pl.pallas_call(
        blend_kernel,
        out_shape=[jax.ShapeDtypeStruct((2, BLK, HD), BF16)] * NY,
        in_specs=[SMEM, SMEM] + [VMEM] * 4,
        out_specs=[VMEM] * NY,
        scratch_shapes=[pltpu.VMEM((NB * BLK, HD), BF16)],
        name="blend",
        **params(1 << 28, 3 << 20),
    )(here, beta, query, local, *memory)


def turn_kernel(*refs):
    core = lax.rem(refs[0][0], 2)
    for step in range(NY):
        refs[-1][step] = refs[1 + step][1 - core]


def turn(here, pieces):
    return pl.pallas_call(
        turn_kernel,
        out_shape=jax.ShapeDtypeStruct((NY, BLK, HD), BF16),
        in_specs=[SMEM] + [VMEM] * NY,
        out_specs=VMEM,
        name="turn",
        **params(0, 1 << 18),
    )(here, *pieces)


def project_kernel(*refs):
    spot_ref = refs[0]
    pieces, other, weight = refs[1 : 1 + NY], refs[1 + NY], refs[2 + NY]
    upper, lower = refs[3 + NY : 5 + NY]
    attended = refs[5 + NY]
    core = lax.rem(spot_ref[0], 2)
    for step in range(NY):
        pair = lax.rem(spot_ref[0] // 2 + step, NY) * 2
        start = pl.multiple_of((pair + core) * HD, HD)
        attended[:, pl.ds(start, HD)] = pieces[step][core]
        start = pl.multiple_of((pair + 1 - core) * HD, HD)
        attended[:, pl.ds(start, HD)] = other[step]
    width = upper.shape[1]
    cols = pl.ds(pl.multiple_of(lax.rem(spot_ref[2] + spot_ref[3], 4) * width, width), width)
    whole = jnp.dot(attended[...], weight[:, cols], preferred_element_type=F32)
    upper[...] = whole[: BLK // 2].astype(upper.dtype)
    lower[...] = whole[BLK // 2 :].astype(lower.dtype)


def project(place, pieces, weight, upper, lower):
    width = weight.shape[1] // 4
    return pl.pallas_call(
        project_kernel,
        in_specs=[SMEM] + [VMEM] * (2 + NY),
        out_specs=(VMEM, VMEM),
        scratch_shapes=[pltpu.VMEM((BLK, NB * HD), BF16)],
        out_shape=(
            jax.ShapeDtypeStruct((BLK // 2, width), upper),
            jax.ShapeDtypeStruct((BLK // 2, width), lower),
        ),
        name="project",
        **params(2 * BLK * NB * HD * width, 3 << 20),
    )(place, *pieces, weight)


def finish_kernel(own_up, own_low, up_a, up_b, low_a, low_b, out):
    half = BLK // 2
    out[:half] = (own_up[...] + up_a[...].astype(F32) + up_b[...].astype(F32)).astype(BF16)
    out[half:] = (own_low[...] + low_a[...].astype(F32) + low_b[...].astype(F32)).astype(BF16)


def finish(*parts):
    return pl.pallas_call(
        finish_kernel,
        in_specs=[VMEM] * 6,
        out_specs=VMEM,
        out_shape=jax.ShapeDtypeStruct((BLK, parts[0].shape[1]), BF16),
        name="finish",
        **params(0, 3 << 20),
    )(*parts)


def layer(queries, keys, values, beta, w_out):
    here = lax.axis_index(PLANE)
    segment = lax.axis_index("seq_0")
    column = lax.axis_index("head")

    def place(e):
        return jnp.stack((here, segment, column, e)).astype(jnp.int32)

    keys, values, queries, w_out = (
        pltpu.with_memory_space_constraint(part, pltpu.HBM)
        for part in (keys, values, queries, w_out)
    )
    stay, leave = split_heads(place(0), keys, values, queries)
    got = shifted(leave, "seq_2", 1)
    kvs, qs = map(list, pair_up(place(0), stay, got))
    past = [shifted(kvs[0], "seq_0", 1)]
    for step in STEPS:
        kvs[step] = shifted(kvs[step], "seq_1", step)
    past.append(shifted(pack(kvs[1], kvs[3]), "seq_0", 1))
    past.append(shifted(kvs[2], "seq_0", 1))
    for step in STEPS:
        qs[step] = shifted(qs[step], "seq_1", step)

    terms, wire = memory_terms(kvs)
    after = shifted(wire, "seq_0", -1)
    chosen, kept = prefix_step(place(0), terms, after)
    after = shifted(chosen, "seq_0", -2)
    window, wire = window_step(kept, after)
    after = shifted(wire, "seq_0", -4)

    k_all, v_all, q_all, acc_a, peak_a = own_first(place(0), kvs, qs)
    acc_b, peak_b = own_second(k_all, v_all, q_all)
    own = (acc_a, peak_a, acc_b, peak_b)
    local, weight = past_part(place(0), past, q_all, own, w_out)
    attended = blend(place(0), beta, q_all, local, (window, after))
    heads = list(attended)
    for step in LEAVE:
        heads[step] = shifted(heads[step], "seq_1", -step)
    heads.append(shifted(turn(place(0), heads), "seq_2", 1))

    def send(part, distance):
        return shifted(part, "head", distance)

    far_up, far_low = project(place(2), heads, weight, BF16, BF16)
    far_up, far_low = send(far_up, 1), send(far_low, -1)
    right_up, right_low = project(place(1), heads, weight, F32, BF16)
    got_low = send(right_low, 1)
    left_up, left_low = project(place(3), heads, weight, BF16, F32)
    got_up = send(left_up, -1)
    more_up = send(added(right_up, far_up, BF16), 1)
    more_low = send(added(left_low, far_low, BF16), -1)
    own_up, own_low = project(place(0), heads, weight, F32, F32)
    return finish(own_up, own_low, got_up, more_up, got_low, more_low)


def solution(mesh):
    torus = Mesh(
        mesh.devices.reshape(8, 4, 2, mesh.shape["head"]), ("seq_0", "seq_1", "seq_2", "head")
    )
    seq = ("seq_0", "seq_1", "seq_2")
    return jax.shard_map(
        layer,
        mesh=torus,
        in_specs=(P(seq, "head"), P(seq, "head"), P(seq, "head"), P("head"), P("head", None)),
        out_specs=P(seq, "head"),
        check_vma=False,
    )
```

```python
import jax
import jax.numpy as jnp
from jax import lax
from jax.experimental import pallas as pl
from jax.experimental.pallas import tpu as pltpu
from jax.sharding import Mesh
from jax.sharding import PartitionSpec as P


HD = 128
BLK = 256
NB = 8
PLANE = ("seq_1", "seq_2")
SCALE2 = (HD**-0.5) * 1.4426950408889634
F32 = jnp.float32
BF16 = jnp.bfloat16
ANY = pl.BlockSpec(memory_space=pl.ANY)
SMEM = pl.BlockSpec(memory_space=pltpu.SMEM)
VMEM = pl.BlockSpec(memory_space=pltpu.VMEM)
HBM = pl.BlockSpec(memory_space=pltpu.HBM)
NY = 4
PAIR = 2 * BLK
STEPS = (1, 3, 2)
LEAVE = (2, 1, 3)
SPLIT = 6


def shifted(block, axis, distance, wrap=True):
    size = lax.axis_size(axis)
    if wrap:
        route = [(i, (i + distance) % size) for i in range(size)]
    else:
        route = [(i, i + distance) for i in range(size - distance)]
    return lax.ppermute(block, axis, route)


def elu_plus(inputs):
    return jnp.where(inputs > 0, inputs + 1.0, jnp.exp(jnp.minimum(inputs, 0.0)))


def pair_rows(here, step, half):
    row = lax.rem(here // 2 - step + NY, NY) * PAIR + half * BLK
    return pl.ds(pl.multiple_of(row, BLK), BLK)


def params(flops, nbytes, room=16):
    return dict(
        cost_estimate=pl.CostEstimate(flops=flops, bytes_accessed=nbytes, transcendentals=0),
        compiler_params=pltpu.CompilerParams(vmem_limit_bytes=room * 1024 * 1024),
    )


def split_kernel(here_ref, keys, values, queries, whole, leave, sems):
    here = here_ref[0]
    copies = [
        pltpu.make_async_copy(array, whole.at[n], sems.at[n])
        for n, array in enumerate((keys, values, queries))
    ]
    for copy in copies:
        copy.start()
    own_core = lax.rem(here, 2)
    for n, copy in enumerate(copies):
        copy.wait()
        for step in range(NY):
            pair = lax.rem(here // 2 + step, NY) * 2
            cols = pl.ds(pl.multiple_of((pair + 1 - own_core) * HD, HD), HD)
            leave[step, n] = whole[n, :, cols]


def split_heads(here, keys, values, queries):
    return pl.pallas_call(
        split_kernel,
        out_shape=(
            jax.ShapeDtypeStruct((3, BLK, NB * HD), BF16),
            jax.ShapeDtypeStruct((NY, 3, BLK, HD), BF16),
        ),
        in_specs=[SMEM] + [HBM] * 3,
        out_specs=(VMEM, VMEM),
        scratch_shapes=[pltpu.SemaphoreType.DMA((3,))],
        name="split",
        **params(0, 3 << 20),
    )(here, keys, values, queries)


def pair_kernel(*refs):
    here_ref, whole, got = refs[:3]
    kvs, qs = refs[3 : 3 + NY], refs[3 + NY : 3 + 2 * NY]
    core = lax.rem(here_ref[0], 2)
    for step in range(NY):
        pair = lax.rem(here_ref[0] // 2 + step, NY) * 2
        cols = pl.ds(pl.multiple_of((pair + core) * HD, HD), HD)
        kvs[step][core] = whole[0:2, :, cols]
        qs[step][core] = whole[2, :, cols]
        kvs[step][1 - core] = got[step, 0:2]
        qs[step][1 - core] = got[step, 2]


def pair_up(here, stay, got):
    out = pl.pallas_call(
        pair_kernel,
        out_shape=[jax.ShapeDtypeStruct((2, 2, BLK, HD), BF16)] * NY
        + [jax.ShapeDtypeStruct((2, BLK, HD), BF16)] * NY,
        in_specs=[SMEM, VMEM, VMEM],
        out_specs=[VMEM] * (2 * NY),
        name="pair_up",
        **params(0, 3 << 20),
    )(here, stay, got)
    return out[:NY], out[NY:]


def pack_kernel(first, second, out):
    out[0] = first[...]
    out[1] = second[...]


def pack(first, second):
    return pl.pallas_call(
        pack_kernel,
        out_shape=jax.ShapeDtypeStruct((2, *first.shape), BF16),
        in_specs=[VMEM, VMEM],
        out_specs=VMEM,
        name="pack",
        **params(0, 1 << 20),
    )(first, second)


def terms_kernel(*refs):
    pieces, out, wire = refs[:NY], refs[NY], refs[NY + 1]
    outer = jnp.zeros((HD, HD), F32)
    totals = jnp.zeros((8, HD), F32)
    for piece in pieces:
        for half in range(2):
            soft = elu_plus(piece[half, 0].astype(F32)).astype(BF16)
            outer = outer + lax.dot_general(
                soft, piece[half, 1], (((0,), (0,)), ((), ())), preferred_element_type=F32
            )
            totals = totals + jnp.dot(jnp.ones((8, BLK), BF16), soft, preferred_element_type=F32)
    out[0:HD, :] = outer
    out[HD : HD + 8, :] = totals
    wire[0:HD, :] = outer.astype(BF16)
    wire[HD : HD + 8, :] = totals.astype(BF16)


def memory_terms(pieces):
    return pl.pallas_call(
        terms_kernel,
        out_shape=(
            jax.ShapeDtypeStruct((HD + 8, HD), F32),
            jax.ShapeDtypeStruct((HD + 8, HD), BF16),
        ),
        in_specs=[VMEM] * NY,
        out_specs=(VMEM, VMEM),
        name="terms",
        **params(2 * 2048 * HD * HD, 1 << 20),
    )(*pieces)


def attend(query, keys, values_ones, scores, first, count, mask_at, mask, start_max=None):
    peak = start_max
    for j in range(count):
        rows = pl.ds((first + j) * BLK, BLK)
        part = lax.dot_general(
            query, keys[rows, :], (((1,), (1,)), ((), ())), preferred_element_type=F32
        )
        if j == mask_at:
            part = jnp.where(mask, part, -jnp.inf)
        scores[:, j * BLK : (j + 1) * BLK] = part
        high = jnp.maximum(part[:, :HD], part[:, HD:])
        peak = high if peak is None else jnp.maximum(peak, high)
    peak = jnp.max(peak, axis=1, keepdims=True)
    half = query.shape[0] // 2
    upper = lower = None
    for j in range(count):
        rows = pl.ds((first + j) * BLK, BLK)
        weights = scores[:, j * BLK : (j + 1) * BLK] - peak
        weights = jnp.exp2(weights * SCALE2).astype(BF16)
        value = values_ones[rows, :]
        above = jnp.dot(weights[:half], value, preferred_element_type=F32)
        below = jnp.dot(weights[half:], value, preferred_element_type=F32)
        upper = above if upper is None else upper + above
        lower = below if lower is None else lower + below
    acc = jnp.concatenate([upper, lower], axis=0)
    return acc, peak


def tile_mask():
    row = lax.broadcasted_iota(jnp.int32, (BLK, BLK), 0)
    col = lax.broadcasted_iota(jnp.int32, (BLK, BLK), 1)
    return col <= row


def own_blocks(blocks, query, keys, values, scores, acc_out, peak_out):
    mask = tile_mask()
    for n, b in enumerate(blocks):
        acc, peak = attend(
            query[pl.ds(b * BLK, BLK), :], keys, values, scores[n % 2], 0, b + 1, b, mask
        )
        rows = pl.ds(n * BLK, BLK)
        acc_out[rows, :] = acc
        peak_out[rows, :] = jnp.broadcast_to(peak, (BLK, HD))


def own_first_kernel(*refs):
    here_ref, kvs, qs = refs[0], refs[1 : 1 + NY], refs[1 + NY : 1 + 2 * NY]
    keys, values, query, acc_out, peak_out = refs[1 + 2 * NY : 6 + 2 * NY]
    scores_a, scores_b = refs[6 + 2 * NY :]
    here = here_ref[0]
    for step in range(NY):
        for half in range(2):
            rows = pair_rows(here, step, half)
            keys[rows, :] = kvs[step][half, 0]
            values[rows, :HD] = kvs[step][half, 1]
            query[rows, :] = qs[step][half]
    values[:, HD:] = jnp.ones((NB * BLK, HD), BF16)
    own_blocks(range(SPLIT), query, keys, values, (scores_a, scores_b), acc_out, peak_out)


def own_second_kernel(keys, values, query, acc_out, peak_out, scores_a, scores_b):
    own_blocks(range(SPLIT, NB), query, keys, values, (scores_a, scores_b), acc_out, peak_out)


def own_first(here, kvs, qs):
    rows = NB * BLK
    return pl.pallas_call(
        own_first_kernel,
        out_shape=(
            jax.ShapeDtypeStruct((rows, HD), BF16),
            jax.ShapeDtypeStruct((rows, 2 * HD), BF16),
            jax.ShapeDtypeStruct((rows, HD), BF16),
            jax.ShapeDtypeStruct((SPLIT * BLK, 2 * HD), F32),
            jax.ShapeDtypeStruct((SPLIT * BLK, HD), F32),
        ),
        in_specs=[SMEM] + [VMEM] * (2 * NY),
        out_specs=(VMEM,) * 5,
        scratch_shapes=[
            pltpu.VMEM((BLK, SPLIT * BLK), F32),
            pltpu.VMEM((BLK, SPLIT * BLK), F32),
        ],
        name="own_first",
        **params(21 * BLK * BLK * HD * 8, 5 << 20),
    )(here, *kvs, *qs)


def own_second(keys, values, query):
    rows = NB * BLK
    return pl.pallas_call(
        own_second_kernel,
        out_shape=(
            jax.ShapeDtypeStruct((rows - SPLIT * BLK, 2 * HD), F32),
            jax.ShapeDtypeStruct((rows - SPLIT * BLK, HD), F32),
        ),
        in_specs=[VMEM] * 3,
        out_specs=(VMEM, VMEM),
        scratch_shapes=[pltpu.VMEM((BLK, rows), F32)] * 2,
        name="own_second",
        **params(15 * BLK * BLK * HD * 8, 3 << 20),
    )(keys, values, query)


def prefix_kernel(place_ref, terms, after, chosen, kept):
    segment = place_ref[1]
    passed = after[...].astype(F32)
    whole = terms[...] + passed
    wrapped = jnp.where(segment == 7, passed, 0.0)
    chosen[...] = jnp.where(segment <= 5, whole, wrapped).astype(BF16)
    kept[...] = jnp.where(segment <= 3, whole, wrapped)


def prefix_step(place, terms, after):
    shape = jax.ShapeDtypeStruct(terms.shape, F32)
    return pl.pallas_call(
        prefix_kernel,
        out_shape=(jax.ShapeDtypeStruct(terms.shape, BF16), shape),
        in_specs=[SMEM, VMEM, VMEM],
        out_specs=(VMEM, VMEM),
        name="prefix",
        **params(0, 1 << 18),
    )(place, terms, after)


def window_kernel(kept, after, out, wire):
    out[...] = kept[...] + after[...].astype(F32)
    wire[...] = out[...].astype(BF16)


def window_step(kept, after):
    return pl.pallas_call(
        window_kernel,
        out_shape=(
            jax.ShapeDtypeStruct(kept.shape, F32),
            jax.ShapeDtypeStruct(kept.shape, BF16),
        ),
        in_specs=[VMEM, VMEM],
        out_specs=(VMEM, VMEM),
        name="window",
        **params(0, 1 << 18),
    )(kept, after)


def add_kernel(left, right, out):
    out[...] = (left[...] + right[...].astype(F32)).astype(out.dtype)


def added(left, right, dtype):
    return pl.pallas_call(
        add_kernel,
        out_shape=jax.ShapeDtypeStruct(left.shape, dtype),
        in_specs=[VMEM, VMEM],
        out_specs=VMEM,
        name="added",
        **params(0, 1 << 18),
    )(left, right)


def past_kernel(*refs):
    here_ref, same, near, far, query = refs[:5]
    acc_a, peak_a, acc_b, peak_b, weight, local_out, weight_out = refs[5:12]
    keys, values, scores_a, scores_b, acc_buf, sem = refs[12:]
    fetch = pltpu.make_async_copy(weight, weight_out, sem)
    fetch.start()
    here, segment = here_ref[0], here_ref[1]

    def own(b):
        if b < SPLIT:
            rows = pl.ds(b * BLK, BLK)
            return acc_a, peak_a, rows
        return acc_b, peak_b, pl.ds((b - SPLIT) * BLK, BLK)

    @pl.when(segment == 0)
    def _():
        acc_buf[: SPLIT * BLK, :] = acc_a[...]
        acc_buf[SPLIT * BLK :, :] = acc_b[...]

    @pl.when(segment > 0)
    def _():
        for step, part in ((0, same), (1, near.at[0]), (3, near.at[1]), (2, far)):
            for half in range(2):
                rows = pair_rows(here, step, half)
                keys[rows, :] = part[half, 0]
                values[rows, :HD] = part[half, 1]
        values[:, HD:] = jnp.ones((NB * BLK, HD), BF16)
        mask = jnp.logical_not(tile_mask())
        for b in range(NB):
            rows = pl.ds(b * BLK, BLK)
            acc_in, peak_in, own_rows = own(b)
            before = peak_in[own_rows, :]
            acc, peak = attend(
                query[rows, :],
                keys,
                values,
                (scores_a, scores_b)[b % 2],
                b,
                NB - b,
                0,
                mask,
                before,
            )
            fade = jnp.exp2((before - peak) * SCALE2)
            acc_buf[rows, :HD] = acc[:, :HD] + acc_in[own_rows, :HD] * fade
            acc_buf[rows, HD:] = acc[:, HD:] + acc_in[own_rows, HD:] * fade

    local_out[...] = acc_buf[:, :HD] / acc_buf[:, HD:]
    fetch.wait()


def blend_kernel(*refs):
    here_ref, beta_ref, query, local_ref, memory_ref, more_ref = refs[:6]
    outs, result = refs[6:-1], refs[-1]
    here, segment = here_ref[0], here_ref[1]
    total = jnp.where(segment <= 3, 0.0, memory_ref[...]) + more_ref[...].astype(F32)
    memory = total[0:HD, :]
    norm = jnp.transpose(jnp.broadcast_to(total[HD : HD + 1, :], (HD, HD)))
    whole = jnp.concatenate([memory, norm], axis=1)
    upper = whole.astype(BF16)
    lower = (whole - upper.astype(F32)).astype(BF16)
    split = jnp.concatenate([upper, lower], axis=0)
    gate = 1.0 / (1.0 + jnp.exp(-jnp.full((1, HD), beta_ref[here], F32)))
    for b in range(NB):
        rows = pl.ds(b * BLK, BLK)
        soft = elu_plus(query[rows, :].astype(F32)).astype(BF16)
        both = jnp.dot(jnp.concatenate([soft, soft], axis=1), split, preferred_element_type=F32)
        from_memory = both[:, :HD] / (1.0 + both[:, HD:])
        local = local_ref[rows, :]
        result[rows, :] = (gate * from_memory + (1.0 - gate) * local).astype(BF16)
    for step in range(NY):
        for half in range(2):
            outs[step][half] = result[pair_rows(here, step, half), :]


def past_part(here, past, query, own, weight):
    rows = NB * BLK
    return pl.pallas_call(
        past_kernel,
        out_shape=(
            jax.ShapeDtypeStruct((rows, HD), F32),
            jax.ShapeDtypeStruct(weight.shape, BF16),
        ),
        in_specs=[SMEM] + [VMEM] * 8 + [HBM],
        out_specs=(VMEM, VMEM),
        scratch_shapes=[
            pltpu.VMEM((rows, HD), BF16),
            pltpu.VMEM((rows, 2 * HD), BF16),
            pltpu.VMEM((BLK, rows), F32),
            pltpu.VMEM((BLK, rows), F32),
            pltpu.VMEM((rows, 2 * HD), F32),
            pltpu.SemaphoreType.DMA,
        ],
        name="past",
        **params(36 * BLK * BLK * HD * 8, 6 << 20, 24),
    )(here, *past, query, *own, weight)


def blend(here, beta, query, local, memory):
    return pl.pallas_call(
        blend_kernel,
        out_shape=[jax.ShapeDtypeStruct((2, BLK, HD), BF16)] * NY,
        in_specs=[SMEM, SMEM] + [VMEM] * 4,
        out_specs=[VMEM] * NY,
        scratch_shapes=[pltpu.VMEM((NB * BLK, HD), BF16)],
        name="blend",
        **params(1 << 28, 3 << 20),
    )(here, beta, query, local, *memory)


def turn_kernel(*refs):
    core = lax.rem(refs[0][0], 2)
    for step in range(NY):
        refs[-1][step] = refs[1 + step][1 - core]


def turn(here, pieces):
    return pl.pallas_call(
        turn_kernel,
        out_shape=jax.ShapeDtypeStruct((NY, BLK, HD), BF16),
        in_specs=[SMEM] + [VMEM] * NY,
        out_specs=VMEM,
        name="turn",
        **params(0, 1 << 18),
    )(here, *pieces)


def project_kernel(*refs):
    spot_ref = refs[0]
    pieces, other, weight = refs[1 : 1 + NY], refs[1 + NY], refs[2 + NY]
    upper, lower = refs[3 + NY : 5 + NY]
    attended = refs[5 + NY]
    core = lax.rem(spot_ref[0], 2)
    for step in range(NY):
        pair = lax.rem(spot_ref[0] // 2 + step, NY) * 2
        start = pl.multiple_of((pair + core) * HD, HD)
        attended[:, pl.ds(start, HD)] = pieces[step][core]
        start = pl.multiple_of((pair + 1 - core) * HD, HD)
        attended[:, pl.ds(start, HD)] = other[step]
    width = upper.shape[1]
    cols = pl.ds(pl.multiple_of(lax.rem(spot_ref[2] + spot_ref[3], 4) * width, width), width)
    whole = jnp.dot(attended[...], weight[:, cols], preferred_element_type=F32)
    upper[...] = whole[: BLK // 2].astype(upper.dtype)
    lower[...] = whole[BLK // 2 :].astype(lower.dtype)


def project(place, pieces, weight, upper, lower):
    width = weight.shape[1] // 4
    return pl.pallas_call(
        project_kernel,
        in_specs=[SMEM] + [VMEM] * (2 + NY),
        out_specs=(VMEM, VMEM),
        scratch_shapes=[pltpu.VMEM((BLK, NB * HD), BF16)],
        out_shape=(
            jax.ShapeDtypeStruct((BLK // 2, width), upper),
            jax.ShapeDtypeStruct((BLK // 2, width), lower),
        ),
        name="project",
        **params(2 * BLK * NB * HD * width, 3 << 20),
    )(place, *pieces, weight)


def finish_kernel(own_up, own_low, up_a, up_b, low_a, low_b, out):
    half = BLK // 2
    out[:half] = (own_up[...] + up_a[...].astype(F32) + up_b[...].astype(F32)).astype(BF16)
    out[half:] = (own_low[...] + low_a[...].astype(F32) + low_b[...].astype(F32)).astype(BF16)


def finish(*parts):
    return pl.pallas_call(
        finish_kernel,
        in_specs=[VMEM] * 6,
        out_specs=VMEM,
        out_shape=jax.ShapeDtypeStruct((BLK, parts[0].shape[1]), BF16),
        name="finish",
        **params(0, 3 << 20),
    )(*parts)


def layer(queries, keys, values, beta, w_out):
    here = lax.axis_index(PLANE)
    segment = lax.axis_index("seq_0")
    column = lax.axis_index("head")

    def place(e):
        return jnp.stack((here, segment, column, e)).astype(jnp.int32)

    keys, values, queries, w_out = (
        pltpu.with_memory_space_constraint(part, pltpu.HBM)
        for part in (keys, values, queries, w_out)
    )
    stay, leave = split_heads(place(0), keys, values, queries)
    got = shifted(leave, "seq_2", 1)
    kvs, qs = map(list, pair_up(place(0), stay, got))
    past = [shifted(kvs[0], "seq_0", 1)]
    for step in STEPS:
        kvs[step] = shifted(kvs[step], "seq_1", step)
    past.append(shifted(pack(kvs[1], kvs[3]), "seq_0", 1))
    past.append(shifted(kvs[2], "seq_0", 1))
    for step in STEPS:
        qs[step] = shifted(qs[step], "seq_1", step)

    terms, wire = memory_terms(kvs)
    after = shifted(wire, "seq_0", -1)
    chosen, kept = prefix_step(place(0), terms, after)
    after = shifted(chosen, "seq_0", -2)
    window, wire = window_step(kept, after)
    after = shifted(wire, "seq_0", -4)

    k_all, v_all, q_all, acc_a, peak_a = own_first(place(0), kvs, qs)
    acc_b, peak_b = own_second(k_all, v_all, q_all)
    own = (acc_a, peak_a, acc_b, peak_b)
    local, weight = past_part(place(0), past, q_all, own, w_out)
    attended = blend(place(0), beta, q_all, local, (window, after))
    heads = list(attended)
    for step in LEAVE:
        heads[step] = shifted(heads[step], "seq_1", -step)
    heads.append(shifted(turn(place(0), heads), "seq_2", 1))

    def send(part, distance):
        return shifted(part, "head", distance)

    far_up, far_low = project(place(2), heads, weight, BF16, BF16)
    far_up, far_low = send(far_up, 1), send(far_low, -1)
    right_up, right_low = project(place(1), heads, weight, F32, BF16)
    got_low = send(right_low, 1)
    left_up, left_low = project(place(3), heads, weight, BF16, F32)
    got_up = send(left_up, -1)
    more_up = send(added(right_up, far_up, BF16), 1)
    more_low = send(added(left_low, far_low, BF16), -1)
    own_up, own_low = project(place(0), heads, weight, F32, F32)
    return finish(own_up, own_low, got_up, more_up, got_low, more_low)


def solution(mesh):
    torus = Mesh(
        mesh.devices.reshape(8, 4, 2, mesh.shape["head"]), ("seq_0", "seq_1", "seq_2", "head")
    )
    seq = ("seq_0", "seq_1", "seq_2")
    return jax.shard_map(
        layer,
        mesh=torus,
        in_specs=(P(seq, "head"), P(seq, "head"), P(seq, "head"), P("head"), P("head", None)),
        out_specs=P(seq, "head"),
        check_vma=False,
    )
```
